32 devices in a mesh: groups: 2 (over y), gx: 16 (over z, x, core).
Axes of the slice: x: 2, y: 2, z: 4, core: 2. Of those that a mesh axis runs over, the one named last changes fastest.
Arguments:
- initial: float32 [20, 4, 256, 1024], P('groups', None, 'gx'), parts along dimension 0, may hold values from -6 to 6
- background: float32 [20, 4, 256, 1024], P('groups', None, 'gx'), parts along dimension 0, may hold values from -6.5 to 6.5
- mixing: float32 [40, 40], replicated, may hold values from -1 to 1
- diffusion: float32 [10, 4], replicated, may hold values from 0.03 to 0.2
- advection: float32 [2, 10, 4], replicated, may hold values from -0.1 to 0.1
- obs_values: float32 [4, 4096], P('groups', 'gx'), parts along dimension 0, may hold values from -6 to 6
- obs_weight: float32 [2, 4096], P('groups', 'gx'), parts along dimension 0, may hold values from 0.5 to 4
- interp_weights: float32 [8, 4096], P('groups', 'gx'), parts along dimension 0, may hold values from 0.1 to 1
- stencil_index: int32 [8, 4096], P('groups', 'gx'), parts along dimension 0, may hold values from 0 to 655359, as said below
- station_tile: int32 [4096, 2], P('gx', 'groups'), parts along dimension 1, may hold values from 0 to 15; in each aligned block of 256 rows (0 to 255, 256 to 511, ...) at most 24 rows name the same one
- counts: int32 [2, 16], P('groups', 'gx'), parts along dimension 0, may hold values from 1 to 256, 3072 in all within a row
Outputs:
- gradient: float32 [20, 4, 256, 1024], P('groups', None, 'gx'), parts along dimension 0
The draws below stay inside these ranges and needn't reach their ends.
There are 2 independent parts, one for each index of `groups`. The reference program is written for one: setup_inputs(seed, part) draws one part's arguments, and reference() takes and returns one part's arrays. A program takes and returns all parts, laid end to end along the dimension named above; an argument that names none is the same for every part. Nothing has to cross between parts.
Inputs may be any that keep to these rules, and one draw needn't show every extreme that they name: `station_tile`: within the rows of one device, no tile is named more than 24 times; some tile is named exactly 24 times in some or all devices' rows. Live observations of a tile occupy its first counts slots; some tile has 256. `stencil_index`: each column holds four cells of one channel of the owner tile, a cell being (channel * 16 + row) * 1024 + column: (row, column), (row, column + 1), (row + 1, column), (row + 1, column + 1) in that order.
All inputs are finite; a program needn't handle non-finite values. No bound on the sum of `counts` on one device may be relied on, other than what follows from the above.
Results may differ from the reference program's by a relative error of at most 0.00014.
Values sent between devices are 32-bit elements; how exact they have to be, the bound alone decides.
No kernel may reach another device: no remote copies, remote signals or barrier semaphores. Data moves between devices by JAX's collectives and lax.ppermute only.
A program may use at most 64 MiB of HBM per device.

```python
import math
import jax
import jax.numpy as jnp
import numpy as np
from jax import lax

F = 10
L = 4
NY = 1024
CX = 16
OBS_DEV = 256
NX = 256
OBS_TOTAL = 4096
CAP = 24
N_GX = 16


def base_state(key):
    state_key = jax.random.fold_in(key, 11)
    raw = jnp.clip(jax.random.normal(state_key, (F, L, NX, NY), jnp.float32), -6.0, 6.0)
    return raw


def draw_initial(key, part):
    return base_state(key).astype(jnp.float32)


def draw_background(key, part):
    step_key = jax.random.fold_in(key, 12)
    increment = 0.1 * jnp.clip(jax.random.normal(step_key, (F, L, NX, NY), jnp.float32), -4.0, 4.0)
    return (base_state(key) + increment).astype(jnp.float32)


def draw_stencil_index(key, part):
    keys = jax.random.split(key, 3)
    channel = jax.random.randint(keys[0], (OBS_TOTAL,), 0, F * L)
    row_start = jax.random.randint(keys[1], (OBS_TOTAL,), 0, CX - 1)
    col_start = jax.random.randint(keys[2], (OBS_TOTAL,), 0, NY - 1)
    base_cell = (channel * CX + row_start) * NY + col_start
    offsets = jnp.array([0, 1, NY, NY + 1], jnp.int32)
    return (base_cell[None, :] + offsets[:, None]).astype(jnp.int32)


def block_levels(stream_key, dims, pieces, low, top_value):
    factor_of = 1.0
    for axis_at, shards_of in pieces:
        draws = jax.random.uniform(jax.random.fold_in(jax.random.fold_in(stream_key, 6), axis_at), (shards_of,), jnp.float32, low / len(pieces), top_value / len(pieces))
        factor_of = factor_of * jnp.repeat(jnp.exp(draws), dims[axis_at] // shards_of).reshape((-1,) + (1,) * (len(dims) - 1 - axis_at))
    return factor_of


def length_profile(amount, total, limit, lean):
    loads = [(1 << 20) // math.isqrt(standing ** lean) + 1 for standing in range(2, amount + 1)]
    spare, given = total - limit - (amount - 1), [1] * (amount - 1)
    while spare > 0:
        free = [i for i in range(amount - 1) if given[i] < limit]
        mass, budget = sum([loads[i] for i in free]), spare
        for i in free:
            extra = min(limit - given[i], max(1, budget * loads[i] // mass), spare)
            given[i] = given[i] + extra
            spare = spare - extra
    return np.array([limit] + given)


def uneven_parts(key, amount, total, most, skew):
    if amount == 2:
        one = jax.random.randint(key, (), max(1, total - most), min(most, total - 1) + 1)
        return jnp.stack([one, total - one])
    sizes = jnp.asarray(length_profile(amount, total, most, skew), jnp.int32)
    twos = (amount - 1) // 2
    source_of, sink = sizes[1:1 + 2 * twos:2], sizes[2:2 + 2 * twos:2]
    slack = jnp.minimum(source_of - 1, most - sink)
    passed = jax.random.randint(jax.random.fold_in(key, 1), (twos,), 0, 1 << 20) % (slack + 1)
    sizes = sizes.at[1:1 + 2 * twos:2].set(source_of - passed).at[2:2 + 2 * twos:2].set(sink + passed)
    return sizes[jax.random.permutation(jax.random.fold_in(key, 2), amount)]


def deal_out(stream_key, own, number, rows, count, top, bound, lean):
    sequence = jax.random.permutation(stream_key, count)
    crowded, usual = shares(count, rows * top, bound, lean, True), shares(count, rows * top, bound, lean, False)
    places = jnp.arange(count)

    def named(lengths, turn):
        used = int((lengths > 0).sum())
        fixed = max(1, used // 4)
        moved = fixed + (places - fixed + turn * (used - fixed)) % max(1, count - fixed)
        return jnp.zeros((count,), jnp.int32).at[sequence[jnp.where(places < fixed, places, moved)]].set(jnp.asarray(lengths, jnp.int32))

    lengths = jnp.where(number % 4 == 0, named(crowded, number // 4), named(usual, number - number // 4 - 1))
    mixed = jax.random.permutation(jax.random.fold_in(own, 3), count)
    giver, receiver = mixed[0:count // 2 * 2:2], mixed[1:count // 2 * 2:2]
    room = jnp.minimum(lengths[giver] - 1, bound - lengths[receiver]) // 2
    room = jnp.where((giver == sequence[0]) | (receiver == sequence[0]) | (lengths[receiver] == 0), 0, jnp.maximum(room, 0))
    moved = jax.random.randint(jax.random.fold_in(own, 4), (count // 2,), 0, 1 << 20) % (room + 1)
    lengths = lengths.at[giver].add(-moved).at[receiver].add(moved)
    members = jnp.searchsorted(jnp.cumsum(lengths), jnp.arange(rows * top), side="right").astype(jnp.int32)
    grid = members.reshape(top, rows).T
    grid = grid[jax.random.permutation(jax.random.fold_in(own, 1), rows)]
    turn = jax.random.randint(jax.random.fold_in(own, 2), (rows, 1), 0, top)
    return jnp.take_along_axis(grid, (jnp.arange(top)[None, :] + turn) % top, axis=1)


def shares(amount, total, limit, lean, full):
    weights = [(1 << 20) // math.isqrt(rank ** lean) + 1 for rank in range(1, amount + 1)]
    largest = limit if full else min(limit, max(-(-total // amount), total * weights[0] // sum(weights)))
    least = 1 if total - largest >= amount - 1 else 0
    given, spare = [largest] + [least] * (amount - 1), total - largest - least * (amount - 1)
    while spare > 0:
        free = [i for i in range(1, amount) if given[i] < largest] or [i for i in range(1, amount) if given[i] < limit]
        pool, left = sum([weights[i] for i in free]), spare
        for i in free:
            extra = min(limit - given[i], max(1, left * weights[i] // pool), spare)
            given[i] = given[i] + extra
            spare = spare - extra
    return np.array(given)


def bell_draw(stream_key, shape, scale, limit, pieces=(), kind=jnp.bfloat16):
    result = jax.random.normal(stream_key, shape, jnp.float32) * scale
    if len(pieces) > 0:
        result = block_levels(stream_key, shape, pieces, -0.22, 0.18) * result
    return jnp.clip(result, min=-limit, max=limit).astype(kind)


def setup_inputs(seed: int = 0, part: int = 0) -> dict:
    key_list = jax.random.split(jax.random.key(seed), 12)
    own_keys = jax.random.split(jax.random.fold_in(key_list[11], part), 12)
    initial = draw_initial(jax.random.fold_in(jax.random.fold_in(key_list[11], part), 71), part)
    background = draw_background(jax.random.fold_in(jax.random.fold_in(key_list[11], part), 71), part)
    mixing = bell_draw(key_list[2], (F * L, F * L), (F * L) ** -0.5, 1.0, (), jnp.float32)
    diffusion = jnp.clip(jnp.exp(jax.random.uniform(key_list[3], (F, L), jnp.float32, math.log(0.03), math.log(0.2))), 0.03, 0.2)
    advection = jnp.clip(jax.random.uniform(key_list[4], (2, F, L), jnp.float32, -0.1, 0.1), -0.1, 0.1)
    obs_values = bell_draw(own_keys[5], (2, OBS_TOTAL), 1.0, 6.0, ((1, 16),), jnp.float32)
    obs_weight = jnp.clip(jnp.exp(math.log(4.0) - 2.0794415 * jax.random.uniform(own_keys[6], (1, OBS_TOTAL), jnp.float32) ** block_levels(own_keys[6], (1, OBS_TOTAL), ((1, 16),), -0.2, 0.2)), 0.5, 4.0)
    interp_weights = jnp.clip(0.1 + 0.9 * jax.random.uniform(own_keys[7], (4, OBS_TOTAL), jnp.float32) ** block_levels(own_keys[7], (4, OBS_TOTAL), ((1, 16),), -0.2, 0.2), 0.1, 1.0)
    stencil_index = draw_stencil_index(jax.random.fold_in(jax.random.fold_in(key_list[11], part), 71), part)
    station_tile_keys = jax.random.split(jax.random.fold_in(own_keys[9], 1), OBS_TOTAL // OBS_DEV)
    station_tile_turns = jax.random.permutation(jax.random.fold_in(own_keys[9], 3), OBS_TOTAL // OBS_DEV)
    station_tile = jax.vmap(lambda own, number: deal_out(jax.random.fold_in(own_keys[9], 2), own, number, OBS_DEV, N_GX, 1, CAP, 2))(station_tile_keys, station_tile_turns).reshape((OBS_TOTAL, 1))
    counts = jax.vmap(lambda own: uneven_parts(own, N_GX, N_GX * OBS_DEV * 3 // 4, OBS_DEV, 2))(jax.random.split(own_keys[10], 1)).reshape((1, N_GX)).astype(jnp.int32)
    return dict(initial=initial, background=background, mixing=mixing, diffusion=diffusion, advection=advection, obs_values=obs_values, obs_weight=obs_weight, interp_weights=interp_weights, stencil_index=stencil_index, station_tile=station_tile, counts=counts)


def tendency(padded, diffuse_rate, drift_x, drift_y):
    centre_cells = padded[:, 1:-1]
    north_side = padded[:, 2:]
    south_side = padded[:, :-2]
    widened = jnp.pad(centre_cells, ((0, 0), (0, 0), (1, 1)))
    east_side = widened[:, :, 2:]
    west_side = widened[:, :, :-2]
    return (diffuse_rate * (north_side + south_side + east_side + west_side - 4.0 * centre_cells)
            + drift_x * (north_side - south_side) + drift_y * (east_side - west_side))


def reference(initial, background, mixing, diffusion, advection, obs_values, obs_weight, interp_weights, stencil_index, station_tile, counts):
    channels = F * L
    start_state = initial.reshape(channels, NX, NY)
    diffuse_rate = diffusion.reshape(channels, 1, 1)
    drift_x = advection[0].reshape(channels, 1, 1)
    drift_y = advection[1].reshape(channels, 1, 1)

    def advance(state):
        padded = jnp.pad(state, ((0, 0), (1, 1), (0, 0)))
        mixed = jnp.einsum("cd,dxy->cxy", mixing, jnp.tanh(state), precision=lax.Precision.HIGHEST)
        return state + tendency(padded, diffuse_rate, drift_x, drift_y) + mixed

    def retreat(cotangent, state):
        padded = jnp.pad(cotangent, ((0, 0), (1, 1), (0, 0)))
        spread = tendency(padded, diffuse_rate, -drift_x, -drift_y)
        back_mix = jnp.einsum("cd,cxy->dxy", mixing, cotangent, precision=lax.Precision.HIGHEST)
        return cotangent + spread + (1.0 - jnp.tanh(state) ** 2) * back_mix

    state_one = advance(start_state)
    state_two = advance(state_one)
    tile_of = station_tile[:, 0]
    channel = stencil_index // (CX * NY)
    remainder = stencil_index % (CX * NY)
    global_cell = (channel * (NX * NY) + tile_of[None, :] * (CX * NY) + remainder).astype(jnp.int32)
    order = jnp.arange(OBS_TOTAL, dtype=jnp.int32)
    alive_mask = (order % OBS_DEV < counts[0, order // OBS_DEV]).astype(jnp.float32)
    weight = obs_weight[0] * alive_mask

    def forcing_at(state, observed):
        flat_state = state.reshape(-1)
        samples = flat_state[global_cell]
        misfit = weight * (jnp.sum(interp_weights * samples, 0) - observed)
        forcing = jnp.zeros((channels * NX * NY,), jnp.float32)
        forcing = forcing.at[global_cell.reshape(-1)].add((misfit[None, :] * interp_weights).reshape(-1))
        return forcing.reshape(channels, NX, NY)

    cot_two = forcing_at(state_two, obs_values[1])
    cot_one = retreat(cot_two, state_one) + forcing_at(state_one, obs_values[0])
    cot_zero = retreat(cot_one, start_state)
    gradient = (start_state - background.reshape(channels, NX, NY)) + cot_zero
    return gradient.reshape(F, L, NX, NY)
```

```python
import functools

import jax
import jax.numpy as jnp
from jax import lax
from jax.experimental import pallas as pl
from jax.experimental.pallas import tpu as pltpu
from jax.sharding import PartitionSpec as P

HALO = 5
LANES = 128
F32, BF16, I32 = jnp.float32, jnp.bfloat16, jnp.int32


def split3(x):
    hi = x.astype(BF16).astype(F32)
    mid = (x - hi).astype(BF16).astype(F32)
    return jnp.concatenate([hi, mid, x - hi - mid], 0).astype(BF16)


def prep_kernel(u_hbm, val, wgt, iw, cell, tile, cnt, up_hbm, dn_hbm, msg, sem, *, n, rows, cols, span):
    copies = []
    for k in range(HALO):
        copies.append(pltpu.make_async_copy(u_hbm.at[:, rows - HALO + k], up_hbm.at[k], sem.at[k]))
        copies.append(pltpu.make_async_copy(u_hbm.at[:, k], dn_hbm.at[k], sem.at[HALO + k]))
    for c in copies:
        c.start()
    held = val.shape[1]
    tgt = jnp.broadcast_to(tile[...], (held, LANES)).T[0:1, :]
    lane = lax.broadcasted_iota(I32, (1, held), 1)
    live = lane < cnt[0, 0]
    base = cell[0:1, :]
    plane = rows * cols
    chan = base // plane
    rest = base - chan * plane
    row = rest // cols
    col = rest - row * cols
    code = (chan * span + row + 4) * cols + col + tgt * plane
    feats = jnp.concatenate([val[...], wgt[...], iw[...], code.astype(F32)], 0)
    feats = split3(feats)
    dest = lax.broadcasted_iota(I32, (n, held), 0)
    hit = (tgt == dest) | ((tgt == dest + 1) & (row <= 1)) | ((tgt == dest - 1) & (row >= rows - 3))
    hit = hit & live
    tri = lax.broadcasted_iota(I32, (held, held), 0) < lax.broadcasted_iota(I32, (held, held), 1)
    hit_f = hit.astype(F32)
    rank = jnp.dot(hit_f.astype(BF16), tri.astype(F32).astype(BF16), preferred_element_type=F32)
    place = jnp.where(hit, rank, -1.0)
    total = jnp.sum(hit_f, axis=1, keepdims=True)
    slot = lax.broadcasted_iota(I32, (LANES, held), 0).astype(F32)
    sub8 = lax.broadcasted_iota(I32, (8, LANES), 0)
    lane8 = lax.broadcasted_iota(I32, (8, LANES), 1)
    for d in range(n):
        pick = (place[d : d + 1, :] == slot).astype(F32).astype(BF16)
        got = lax.dot_general(feats, pick, (((1,), (1,)), ((), ())), preferred_element_type=F32)
        got = got[0:8] + got[8:16] + got[16:24]
        got = jnp.where(sub8 == 7, got - float(d * plane), got)
        msg[d] = jnp.where((sub8 == 7) & (lane8 == LANES - 1), total[d : d + 1, 0:1], got)
    for c in copies:
        c.wait()


def main_kernel(
    edge, dif, adv, u_hbm, b_hbm, up_hbm, dn_hbm, msg_hbm, msg, mix, out_hbm,
    u0, bg, u1, u2, f1, f2, dt0, dt1, stage, tab, table, coef, mats, code_s, list_s,
    sem_u, sem_b, sem_e, sem_o, sem_m, *, n, rows, cols, chans, span,
):
    nf, nl = dif.shape
    load_u = lambda x: pltpu.make_async_copy(u_hbm.at[:, x], u0.at[HALO + x], sem_u.at[x])
    load_b = lambda x: pltpu.make_async_copy(b_hbm.at[:, x], bg.at[x], sem_b.at[x])
    store_o = lambda x: pltpu.make_async_copy(bg.at[x], out_hbm.at[:, x], sem_o.at[x])
    edges = [
        pltpu.make_async_copy(up_hbm, u0.at[pl.ds(0, HALO)], sem_e.at[0]),
        pltpu.make_async_copy(dn_hbm, u0.at[pl.ds(HALO + rows, HALO)], sem_e.at[1]),
    ]
    codes = pltpu.make_async_copy(msg_hbm.at[:, 7], code_s, sem_m)
    codes.start()
    for c in edges:
        c.start()
    for x in range(rows):
        load_u(x).start()
    for x in range(rows):
        load_b(x).start()

    for ch in range(chans):
        i, j = ch // nl, ch % nl
        c, a, b = dif[i, j], adv[0, i, j], adv[1, i, j]
        for k, v in enumerate((c + a, c - a, c + b, c - b, 1.0 - 4.0 * c)):
            coef[k, ch : ch + 1, :] = jnp.full((1, LANES), v, F32)
    mats[...] = jnp.zeros_like(mats)
    m = mix[...]
    mats[2, 0:chans, 0:chans] = m
    mt = mats[2].T[0:chans, 0:chans]
    for k, v in enumerate((m, mt)):
        hi = v.astype(BF16).astype(F32)
        lo = v - hi
        mats[k, 0:chans, 0:chans] = hi
        mats[k, 0:chans, chans : 2 * chans] = hi
        mats[k, chans : 2 * chans, 0:chans] = lo
        mats[k, chans : 2 * chans, chans : 2 * chans] = lo
    fwd = mats[0, 0 : 2 * chans, 0 : 2 * chans].astype(BF16)
    bwd = mats[1, 0 : 2 * chans, 0 : 2 * chans].astype(BF16)

    def mixed(lhs, v):
        hi = v.astype(BF16).astype(F32)
        rhs = jnp.concatenate([hi, v - hi], 0).astype(BF16)
        r = jnp.dot(lhs, rhs, preferred_element_type=F32)
        return r[0:chans] + r[chans : 2 * chans]

    lane = lax.broadcasted_iota(I32, (chans, cols), 1)

    def stencil(north, v, south, sign):
        cn, cs, ce, cw, cc = (jnp.tile(coef[k], (1, cols // LANES)) for k in range(5))
        if sign < 0:
            cn, cs, ce, cw = cs, cn, cw, ce
        east = jnp.where(lane == cols - 1, 0.0, pltpu.roll(v, cols - 1, 1))
        west = jnp.where(lane == 0, 0.0, pltpu.roll(v, 1, 1))
        return cc * v + cn * north + cs * south + ce * east + cw * west

    f1[...] = jnp.zeros_like(f1)
    f2[...] = jnp.zeros_like(f2)

    def spread(s, _):
        tab[pl.ds(s * LANES, LANES), 0:8] = msg[s].T
        return 0

    lax.fori_loop(0, n, spread, 0)
    top, bot = edge[0, 0], edge[0, 1]
    for c in edges:
        c.wait()
    for x in range(rows):
        load_u(x).wait()

    def inside(row):
        return jnp.where(row < 0, top, jnp.where(row >= rows, bot, 1.0))

    def first(k, _):
        v = u0[k + 1]
        t = jnp.tanh(v)
        r = stencil(u0[k + 2], v, u0[k], 1) + mixed(fwd, t)
        u1[k] = r * inside(k - 4)
        dt0[k] = 1.0 - t * t
        return 0

    lax.fori_loop(0, rows + 8, first, 0)

    def second(k, _):
        v = u1[k + 1]
        t = jnp.tanh(v)
        u2[k] = stencil(u1[k + 2], v, u1[k], 1) + mixed(fwd, t)
        dt1[k] = 1.0 - t * t
        return 0

    lax.fori_loop(0, rows + 6, second, 0)

    codes.wait()

    def at(code):
        q = code // cols
        y = code - q * cols
        blk = jnp.minimum(y // LANES, cols // LANES - 2)
        return q // span, q % span, pl.multiple_of(blk * LANES, LANES)

    def gather_src(s, off):
        cnt = code_s[s, LANES - 1].astype(I32)

        def one(k, p):
            code = code_s[s, k].astype(I32)
            list_s[p] = code
            ch, x, y = at(code)
            at_ch, at_y, at_p = pl.ds(ch, 1), pl.ds(y, 2 * LANES), pl.ds(p, 1)
            stage[0, at_p] = u1[x, at_ch, at_y]
            stage[1, at_p] = u1[x + 1, at_ch, at_y]
            stage[2, at_p] = u2[x - 1, at_ch, at_y]
            stage[3, at_p] = u2[x, at_ch, at_y]
            table[at_p] = tab[pl.ds(s * LANES + k, 1)]
            return p + 1

        return lax.fori_loop(0, cnt, one, off)

    count = lax.fori_loop(0, n, gather_src, 0)

    lane2 = lax.broadcasted_iota(I32, (8, 2 * LANES), 1)

    def misfits(g, _):
        p = pl.multiple_of(g * 8, 8)
        at_p = pl.ds(p, 8)
        rec = table[at_p]
        code = rec[:, 7:8].astype(I32)
        y = code - (code // cols) * cols
        l = y - jnp.minimum(y // LANES, cols // LANES - 2) * LANES
        here, nxt = lane2 == l, lane2 == l + 1
        w0 = jnp.where(here, rec[:, 3:4], 0.0) + jnp.where(nxt, rec[:, 4:5], 0.0)
        w1 = jnp.where(here, rec[:, 5:6], 0.0) + jnp.where(nxt, rec[:, 6:7], 0.0)
        w = rec[:, 2:3]
        d1 = w * (jnp.sum(w0 * stage[0, at_p] + w1 * stage[1, at_p], 1, keepdims=True) - rec[:, 0:1])
        d2 = w * (jnp.sum(w0 * stage[2, at_p] + w1 * stage[3, at_p], 1, keepdims=True) - rec[:, 1:2])
        stage[0, at_p] = d1 * w0
        stage[1, at_p] = d1 * w1
        stage[2, at_p] = d2 * w0
        stage[3, at_p] = d2 * w1
        return 0

    lax.fori_loop(0, (count + 7) // 8, misfits, 0)

    def scatter(p, _):
        ch, x, y = at(list_s[p])
        at_ch, at_y, at_p = pl.ds(ch, 1), pl.ds(y, 2 * LANES), pl.ds(p, 1)
        a = f1[x - 1, at_ch, at_y] + stage[0, at_p]
        b = f1[x, at_ch, at_y] + stage[1, at_p]
        c = f2[x - 1, at_ch, at_y] + stage[2, at_p]
        d = f2[x, at_ch, at_y] + stage[3, at_p]
        f1[x - 1, at_ch, at_y] = a
        f1[x, at_ch, at_y] = b
        f2[x - 1, at_ch, at_y] = c
        f2[x, at_ch, at_y] = d
        return 0

    lax.fori_loop(0, count, scatter, 0)

    def third(j, _):
        k = j + 2
        v = f2[k]
        r = stencil(f2[k + 1], v, f2[k - 1], -1) + dt1[k] * mixed(bwd, v) + f1[k]
        f1[k] = r * inside(j - 1)
        return 0

    lax.fori_loop(0, rows + 2, third, 0)
    for x in range(rows):
        load_b(x).wait()

    def fourth(x, _):
        k = x + 3
        v = f1[k]
        r = stencil(f1[k + 1], v, f1[k - 1], -1) + dt0[x + 4] * mixed(bwd, v)
        bg[x] = (u0[x + HALO] - bg[x]) + r
        store_o(x).start()
        return 0

    lax.fori_loop(0, rows, fourth, 0)
    for x in range(rows):
        store_o(x).wait()


def shards(
    initial, background, mixing, diffusion, advection, obs_values, obs_weight, interp_weights,
    stencil_index, station_tile, counts,
):
    fields, levels, rows, cols = initial.shape
    chans = fields * levels
    n = lax.axis_size("gx")
    held = obs_values.shape[1]
    cap = max(2, held * 3 // (2 * n))
    most = -(-3 * cap * n // 8) * 8 + 8
    span = 1 << (rows + 7).bit_length()
    u = initial.reshape(chans, rows, cols)
    b = background.reshape(chans, rows, cols)
    vmem, smem, hbm = (pl.BlockSpec(memory_space=s) for s in (pltpu.VMEM, pltpu.SMEM, pl.ANY))
    edge_shape = jax.ShapeDtypeStruct((HALO, chans, cols), F32)
    up_send, dn_send, msg = pl.pallas_call(
        functools.partial(prep_kernel, n=n, rows=rows, cols=cols, span=span),
        out_shape=(edge_shape, edge_shape, jax.ShapeDtypeStruct((n, 8, LANES), F32)),
        in_specs=[hbm, vmem, vmem, vmem, vmem, vmem, smem],
        out_specs=(hbm, hbm, vmem),
        scratch_shapes=[pltpu.SemaphoreType.DMA((2 * HALO,))],
        name="prep",
    )(u, obs_values, obs_weight, interp_weights, stencil_index, station_tile, counts)
    up = [(i, i + 1) for i in range(n - 1)]
    down = [(j, i) for i, j in up]
    from_up = lax.ppermute(up_send, "gx", up)
    from_dn = lax.ppermute(dn_send, "gx", down)
    msg = lax.all_to_all(msg, "gx", split_axis=0, concat_axis=0, tiled=True)
    me = lax.axis_index("gx")
    edge = jnp.stack([me > 0, me < n - 1]).astype(F32).reshape(1, 2)
    tile = (chans, cols)
    out = pl.pallas_call(
        functools.partial(main_kernel, n=n, rows=rows, cols=cols, chans=chans, span=span),
        out_shape=jax.ShapeDtypeStruct((chans, rows, cols), F32),
        in_specs=[smem, smem, smem, hbm, hbm, hbm, hbm, hbm, vmem, vmem],
        out_specs=hbm,
        scratch_shapes=[
            pltpu.VMEM((rows + 2 * HALO, *tile), F32),
            pltpu.VMEM((rows, *tile), F32),
            pltpu.VMEM((rows + 8, *tile), F32),
            pltpu.VMEM((rows + 6, *tile), F32),
            pltpu.VMEM((rows + 6, *tile), F32),
            pltpu.VMEM((rows + 6, *tile), F32),
            pltpu.VMEM((rows + 8, *tile), F32),
            pltpu.VMEM((rows + 6, *tile), F32),
            pltpu.VMEM((4, most, 2 * LANES), F32),
            pltpu.VMEM((n * LANES, LANES), F32),
            pltpu.VMEM((most, LANES), F32),
            pltpu.VMEM((5, chans, LANES), F32),
            pltpu.VMEM((3, LANES, LANES), F32),
            pltpu.SMEM((n, LANES), F32),
            pltpu.SMEM((most,), I32),
            pltpu.SemaphoreType.DMA((rows,)),
            pltpu.SemaphoreType.DMA((rows,)),
            pltpu.SemaphoreType.DMA((2,)),
            pltpu.SemaphoreType.DMA((rows,)),
            pltpu.SemaphoreType.DMA(()),
        ],
        compiler_params=pltpu.CompilerParams(vmem_limit_bytes=60 * 1024 * 1024),
        name="adjoint",
    )(edge, diffusion, advection, u, b, from_up, from_dn, msg, msg, mixing)
    return out.reshape(fields, levels, rows, cols)


def solution(mesh):
    placed = (
        P("groups", None, "gx", None),
        P("groups", None, "gx", None),
        P(),
        P(),
        P(),
        P("groups", "gx"),
        P("groups", "gx"),
        P("groups", "gx"),
        P("groups", "gx"),
        P("gx", "groups"),
        P("groups", "gx"),
    )
    return jax.shard_map(
        shards, mesh=mesh, in_specs=placed, out_specs=P("groups", None, "gx", None), check_vma=False
    )
```

```python
import functools

import jax
import jax.numpy as jnp
from jax import lax
from jax.experimental import pallas as pl
from jax.experimental.pallas import tpu as pltpu
from jax.sharding import PartitionSpec as P

HALO = 5
LANES = 128
WIDE = 2 * LANES
SUB = 8
F32, BF16, I32 = jnp.float32, jnp.bfloat16, jnp.int32


def split3(x):
    hi = x.astype(BF16).astype(F32)
    mid = (x - hi).astype(BF16).astype(F32)
    return [hi, mid, x - hi - mid]


def prep_kernel(u_hbm, val, wgt, iw, cell, tile, cnt, up, dn, msg, sem, *, n, rows, cols, groups):
    copies = []
    for k in range(HALO):
        at = pl.ds(k * groups, groups)
        copies.append(pltpu.make_async_copy(u_hbm.at[:, :, rows - HALO + k], up.at[at], sem.at[k]))
        copies.append(pltpu.make_async_copy(u_hbm.at[:, :, k], dn.at[at], sem.at[HALO + k]))
    for c in copies:
        c.start()
    held = val.shape[1]
    blocks = cols // LANES
    tgt = tile[...]
    lane = lax.broadcasted_iota(I32, (1, held), 1)
    live = lane < cnt[0, 0]
    base = cell[0:1, :]
    plane = rows * cols
    chan = base // plane
    rest = base - chan * plane
    row = rest // cols
    col = rest - row * cols
    blk = jnp.minimum(col // LANES, blocks - 2)
    line = (row + 4) * groups + chan // SUB
    code = ((line * SUB + chan % SUB) * blocks + blk) * WIDE + col - blk * LANES
    step = rows * groups * SUB * blocks * WIDE
    feats = jnp.concatenate(split3(jnp.concatenate([val[...], wgt[...], iw[...], jnp.zeros((1, held), F32)], 0)), 0)
    pad = jnp.zeros((SUB - 3, held), F32)
    dest = lax.broadcasted_iota(I32, (n, held), 0)
    hit = (tgt == dest) | ((tgt == dest + 1) & (row <= 1)) | ((tgt == dest - 1) & (row >= rows - 3))
    hit = hit & live
    tri = lax.broadcasted_iota(I32, (held, held), 0) < lax.broadcasted_iota(I32, (held, held), 1)
    hit_f = hit.astype(F32)
    rank = jnp.dot(hit_f.astype(BF16), tri.astype(F32).astype(BF16), preferred_element_type=F32)
    place = jnp.where(hit, rank, -1.0)
    total = jnp.sum(hit_f, axis=1, keepdims=True)
    slot = lax.broadcasted_iota(I32, (LANES, held), 0).astype(F32)
    sub8 = lax.broadcasted_iota(I32, (SUB, LANES), 0)
    lane8 = lax.broadcasted_iota(I32, (SUB, LANES), 1)
    least = float(groups * SUB * blocks * WIDE)
    for d in range(n):
        pick = (place[d : d + 1, :] == slot).astype(F32).astype(BF16)
        code_d = (code + (tgt - d) * step).astype(F32)
        lhs = jnp.concatenate([feats, *split3(code_d), pad], 0).astype(BF16)
        got = lax.dot_general(lhs, pick, (((1,), (1,)), ((), ())), preferred_element_type=F32)
        where = jnp.maximum(got[24:25] + got[25:26] + got[26:27], least)
        got = got[0:8] + got[8:16] + got[16:24]
        got = jnp.where(sub8 == 7, where, got)
        msg[d] = jnp.where((sub8 == 7) & (lane8 == LANES - 1), total[d : d + 1, 0:1], got)
    for c in copies:
        c.wait()


def main_kernel(
    dif, adv, u_hbm, b_hbm, up_hbm, dn_hbm, msg, mix, out_hbm,
    u0, bg, u1, u2, f1, f2, dt0, dt1, stage, tab, table, coef, mats, code_v, code_s, list_s,
    sem_u, sem_b, sem_e, sem_o, sem_m, *, n, rows, cols, chans, levels,
):
    groups, blocks = chans // SUB, cols // LANES
    line = lambda ref, x: ref.at[pl.ds(x * groups, groups)]
    load_u = lambda x: pltpu.make_async_copy(u_hbm.at[:, :, x], line(u0, HALO + x), sem_u.at[x])
    load_b = lambda x: pltpu.make_async_copy(b_hbm.at[:, :, x], line(bg, x), sem_b.at[x])
    store_o = lambda x: pltpu.make_async_copy(line(bg, x), out_hbm.at[:, :, x], sem_o.at[x])
    span = HALO * groups
    edges = [
        pltpu.make_async_copy(up_hbm, u0.at[pl.ds(0, span)], sem_e.at[0]),
        pltpu.make_async_copy(dn_hbm, u0.at[pl.ds(span + rows * groups, span)], sem_e.at[1]),
    ]
    for c in edges:
        c.start()
    for x in range(rows):
        load_u(x).start()
    for x in range(rows):
        load_b(x).start()
    code_v[...] = msg[:, SUB - 1, :].astype(I32)
    codes = pltpu.make_async_copy(code_v, code_s, sem_m)
    codes.start()

    for ch in range(chans):
        i, j = ch // levels, ch % levels
        c, a, b = dif[j, i], adv[0, j, i], adv[1, j, i]
        for k, v in enumerate((c + a, c - a, c + b, c - b, 1.0 - 4.0 * c)):
            coef[k, ch : ch + 1, :] = jnp.full((1, LANES), v, F32)
    mats[2] = jnp.zeros_like(mats[2])
    m = mix[...]
    mats[2, 0:chans, 0:chans] = m
    mt = mats[2].T[0:chans, 0:chans]
    for k, v in enumerate((m, mt)):
        hi = v.astype(BF16).astype(F32)
        mats[k, 0:chans, 0:chans] = hi
        mats[k, 0:chans, chans : 2 * chans] = hi
        mats[k, 0:chans, 2 * chans : 3 * chans] = v - hi
    fwd = mats[0, 0:chans, 0 : 3 * chans].astype(BF16)
    bwd = mats[1, 0:chans, 0 : 3 * chans].astype(BF16)
    lane = lax.broadcasted_iota(I32, (chans, LANES), 1)
    zero = jnp.zeros((chans, LANES), F32)

    def get(ref, x, b):
        return ref[pl.ds(x * groups, groups), :, b * LANES : (b + 1) * LANES].reshape(chans, LANES)

    def put(ref, x, b, v):
        ref[pl.ds(x * groups, groups), :, b * LANES : (b + 1) * LANES] = v.reshape(groups, SUB, LANES)

    def mixed(lhs, parts):
        res = []
        for b in range(0, blocks, 2):
            v = jnp.concatenate(parts[b : b + 2], 1)
            hi = v.astype(BF16).astype(F32)
            rhs = jnp.concatenate([hi, v - hi, hi], 0).astype(BF16)
            r = jnp.dot(lhs, rhs, preferred_element_type=F32)
            res += [r[:, :LANES], r[:, LANES:]]
        return res

    def stencil(ref, x, parts, sign):
        kn, ks, ke, kw = (0, 1, 2, 3) if sign > 0 else (1, 0, 3, 2)
        res = []
        left = [pltpu.roll(v, LANES - 1, 1) for v in parts] + [zero]
        right = [zero] + [pltpu.roll(v, 1, 1) for v in parts]
        for b in range(blocks):
            east = jnp.where(lane == LANES - 1, left[b + 1], left[b])
            west = jnp.where(lane == 0, right[b], right[b + 1])
            r = coef[4] * parts[b] + coef[kn] * get(ref, x + 1, b) + coef[ks] * get(ref, x - 1, b)
            res.append(r + coef[ke] * east + coef[kw] * west)
        return res

    def over(count, width, body):
        def several(i, _):
            for r in range(width):
                body(i * width + r)
            return 0

        lax.fori_loop(0, count // width, several, 0)

    f1[...] = jnp.zeros_like(f1)
    f2[...] = jnp.zeros_like(f2)

    def spread(s, _):
        tab[pl.ds(s * LANES, LANES), 0:SUB] = msg[s].T
        return 0

    lax.fori_loop(0, n, spread, 0)
    me = lax.axis_index("gx")
    for c in edges:
        c.wait()
    for x in range(rows):
        load_u(x).wait()

    def first(k):
        v = [get(u0, k + 1, b) for b in range(blocks)]
        t = [jnp.tanh(p) for p in v]
        p = mixed(fwd, t)
        s = stencil(u0, k + 1, v, 1)
        for b in range(blocks):
            put(dt0, k, b, 1.0 - t[b] * t[b])
            put(u1, k, b, s[b] + p[b])

    over(rows + 8, 2, first)

    def clear(ref, x, count):
        ref[pl.ds(x * groups, count * groups)] = jnp.zeros((count * groups, SUB, cols), F32)

    @pl.when(me == 0)
    def _():
        clear(u1, 0, 4)

    @pl.when(me == n - 1)
    def _():
        clear(u1, rows + 4, 4)

    def second(k):
        v = [get(u1, k + 1, b) for b in range(blocks)]
        t = [jnp.tanh(p) for p in v]
        p = mixed(fwd, t)
        s = stencil(u1, k + 1, v, 1)
        for b in range(blocks):
            put(dt1, k, b, 1.0 - t[b] * t[b])
            put(u2, k, b, s[b] + p[b])

    over(rows + 6, 2, second)

    codes.wait()
    unroll = 4
    shift = (WIDE.bit_length() - 1, blocks.bit_length() - 1, SUB.bit_length() - 1)

    def at(code):
        q = lax.shift_right_logical(code, shift[0])
        y = pl.multiple_of(lax.shift_left(q & (blocks - 1), 7), LANES)
        q = lax.shift_right_logical(q, shift[1])
        return lax.shift_right_logical(q, shift[2]), pl.ds(q & (SUB - 1), 1), pl.ds(y, WIDE)

    def gather_src(s, off):
        cnt = code_s[s, LANES - 1]

        def some(i, _):
            for r in range(unroll):
                k = i * unroll + r
                p = off + k
                code = code_s[s, k]
                list_s[p] = code
                x, at_s, at_y = at(code)
                at_p = pl.ds(p, 1)
                stage[0, at_p] = u1[x, at_s, at_y]
                stage[1, at_p] = u1[x + groups, at_s, at_y]
                stage[2, at_p] = u2[x - groups, at_s, at_y]
                stage[3, at_p] = u2[x, at_s, at_y]
                table[at_p] = tab[pl.ds(s * LANES + k, 1)]
            return 0

        lax.fori_loop(0, lax.shift_right_logical(cnt + unroll - 1, 2), some, 0)
        return off + cnt

    count = lax.fori_loop(0, n, gather_src, 0)
    for r in range(unroll):
        list_s[count + r] = groups * SUB * blocks * WIDE

    per = 16
    lane2 = lax.broadcasted_iota(I32, (per, WIDE), 1)
    nth = lax.broadcasted_iota(I32, (per, 1), 0)

    def misfits(g, _):
        p = pl.multiple_of(g * per, per)
        at_p = pl.ds(p, per)
        rec = table[at_p]
        l = rec[:, 7:8].astype(I32) & (WIDE - 1)
        here, nxt = lane2 == l, lane2 == l + 1
        w0 = jnp.where(here, rec[:, 3:4], jnp.where(nxt, rec[:, 4:5], 0.0))
        w1 = jnp.where(here, rec[:, 5:6], jnp.where(nxt, rec[:, 6:7], 0.0))
        w = rec[:, 2:3]
        ok = p + nth < count
        d1 = w * (jnp.sum(w0 * stage[0, at_p] + w1 * stage[1, at_p], 1, keepdims=True) - rec[:, 0:1])
        d2 = w * (jnp.sum(w0 * stage[2, at_p] + w1 * stage[3, at_p], 1, keepdims=True) - rec[:, 1:2])
        stage[0, at_p] = jnp.where(ok, d1 * w0, 0.0)
        stage[1, at_p] = jnp.where(ok, d1 * w1, 0.0)
        stage[2, at_p] = jnp.where(ok, d2 * w0, 0.0)
        stage[3, at_p] = jnp.where(ok, d2 * w1, 0.0)
        return 0

    lax.fori_loop(0, lax.div(count + per - 1, per), misfits, 0)

    def scatter(i, _):
        for r in range(unroll):
            p = i * unroll + r
            x, at_s, at_y = at(list_s[p])
            at_p = pl.ds(p, 1)
            a = f1[x - groups, at_s, at_y] + stage[0, at_p]
            b = f1[x, at_s, at_y] + stage[1, at_p]
            c = f2[x - groups, at_s, at_y] + stage[2, at_p]
            d = f2[x, at_s, at_y] + stage[3, at_p]
            f1[x - groups, at_s, at_y] = a
            f1[x, at_s, at_y] = b
            f2[x - groups, at_s, at_y] = c
            f2[x, at_s, at_y] = d
        return 0

    lax.fori_loop(0, lax.shift_right_logical(count + unroll - 1, 2), scatter, 0)

    def third(j):
        k = j + 2
        v = [get(f2, k, b) for b in range(blocks)]
        p = mixed(bwd, v)
        s = stencil(f2, k, v, -1)
        for b in range(blocks):
            put(f1, k, b, (s[b] + get(f1, k, b)) + get(dt1, k, b) * p[b])

    over(rows + 2, 2, third)

    @pl.when(me == 0)
    def _():
        clear(f1, 2, 1)

    @pl.when(me == n - 1)
    def _():
        clear(f1, rows + 3, 1)

    for x in range(rows):
        load_b(x).wait()

    def fourth(x):
        k = x + 3
        v = [get(f1, k, b) for b in range(blocks)]
        p = mixed(bwd, v)
        s = stencil(f1, k, v, -1)
        for b in range(blocks):
            r = s[b] + get(dt0, x + 4, b) * p[b]
            put(bg, x, b, (get(u0, x + HALO, b) - get(bg, x, b)) + r)
        store_o(x).start()

    over(rows, 2, fourth)
    for x in range(rows):
        store_o(x).wait()


def shards(
    initial, background, mixing, diffusion, advection, obs_values, obs_weight, interp_weights,
    stencil_index, station_tile, counts,
):
    fields, levels, rows, cols = initial.shape
    chans = fields * levels
    groups = chans // SUB
    n = lax.axis_size("gx")
    held = obs_values.shape[1]
    cap = max(2, held * 3 // (2 * n))
    most = -(-3 * cap * n // 16) * 16 + 16
    u = initial.reshape(groups, SUB, rows, cols)
    b = background.reshape(groups, SUB, rows, cols)
    vmem, smem, hbm = (pl.BlockSpec(memory_space=s) for s in (pltpu.VMEM, pltpu.SMEM, pl.ANY))
    edge_shape = jax.ShapeDtypeStruct((HALO * groups, SUB, cols), F32)
    up_send, dn_send, msg = pl.pallas_call(
        functools.partial(prep_kernel, n=n, rows=rows, cols=cols, groups=groups),
        out_shape=(edge_shape, edge_shape, jax.ShapeDtypeStruct((n, SUB, LANES), F32)),
        in_specs=[hbm, vmem, vmem, vmem, vmem, vmem, smem],
        out_specs=(vmem, vmem, vmem),
        scratch_shapes=[pltpu.SemaphoreType.DMA((2 * HALO,))],
        name="prep",
    )(u, obs_values, obs_weight, interp_weights, stencil_index, station_tile.T, counts)
    up = [(i, i + 1) for i in range(n - 1)]
    down = [(j, i) for i, j in up]
    from_up = lax.ppermute(up_send, "gx", up)
    from_dn = lax.ppermute(dn_send, "gx", down)
    msg = lax.all_to_all(msg, "gx", split_axis=0, concat_axis=0, tiled=True)
    buf = lambda count: pltpu.VMEM((count * groups, SUB, cols), F32)
    out = pl.pallas_call(
        functools.partial(main_kernel, n=n, rows=rows, cols=cols, chans=chans, levels=levels),
        out_shape=jax.ShapeDtypeStruct(u.shape, F32),
        in_specs=[smem, smem, hbm, hbm, hbm, hbm, vmem, vmem],
        out_specs=hbm,
        scratch_shapes=[
            buf(rows + 2 * HALO),
            buf(rows),
            buf(rows + 8),
            buf(rows + 6),
            buf(rows + 6),
            buf(rows + 6),
            buf(rows + 8),
            buf(rows + 6),
            pltpu.VMEM((4, most, WIDE), F32),
            pltpu.VMEM((n * LANES, LANES), F32),
            pltpu.VMEM((most, LANES), F32),
            pltpu.VMEM((5, chans, LANES), F32),
            pltpu.VMEM((3, LANES, LANES), F32),
            pltpu.VMEM((n, LANES), I32),
            pltpu.SMEM((n, LANES), I32),
            pltpu.SMEM((most,), I32),
            pltpu.SemaphoreType.DMA((rows,)),
            pltpu.SemaphoreType.DMA((rows,)),
            pltpu.SemaphoreType.DMA((2,)),
            pltpu.SemaphoreType.DMA((rows,)),
            pltpu.SemaphoreType.DMA(()),
        ],
        compiler_params=pltpu.CompilerParams(vmem_limit_bytes=56 * 1024 * 1024),
        name="adjoint",
    )(diffusion.T, advection.transpose(0, 2, 1), u, b, from_up, from_dn, msg, mixing)
    return out.reshape(fields, levels, rows, cols)


def solution(mesh):
    placed = (
        P("groups", None, "gx", None),
        P("groups", None, "gx", None),
        P(),
        P(),
        P(),
        P("groups", "gx"),
        P("groups", "gx"),
        P("groups", "gx"),
        P("groups", "gx"),
        P("gx", "groups"),
        P("groups", "gx"),
    )
    return jax.shard_map(
        shards, mesh=mesh, in_specs=placed, out_specs=P("groups", None, "gx", None), check_vma=False
    )
```

```python
import functools

import jax
import jax.numpy as jnp
from jax import lax
from jax.experimental import pallas as pl
from jax.experimental.pallas import tpu as pltpu
from jax.sharding import PartitionSpec as P

HALO = 5
LANES = 128
WIDE = 2 * LANES
SUB = 8
F32, BF16, I32 = jnp.float32, jnp.bfloat16, jnp.int32


def split3(x):
    hi = x.astype(BF16).astype(F32)
    mid = (x - hi).astype(BF16).astype(F32)
    return [hi, mid, x - hi - mid]


def edges_kernel(u_hbm, up, dn, sem, *, rows, groups):
    copies = []
    for k in range(HALO):
        at = pl.ds(k * groups, groups)
        copies.append(pltpu.make_async_copy(u_hbm.at[:, :, rows - HALO + k], up.at[at], sem.at[k]))
        copies.append(pltpu.make_async_copy(u_hbm.at[:, :, k], dn.at[at], sem.at[HALO + k]))
    for c in copies:
        c.start()
    for c in copies:
        c.wait()


def bucket_kernel(val, wgt, iw, cell, tile, cnt, msg, *, n, rows, cols, groups):
    held = val.shape[1]
    blocks = cols // LANES
    tgt = tile[...]
    lane = lax.broadcasted_iota(I32, (1, held), 1)
    live = lane < cnt[0, 0]
    base = cell[0:1, :]
    plane = rows * cols
    chan = base // plane
    rest = base - chan * plane
    row = rest // cols
    col = rest - row * cols
    blk = jnp.minimum(col // LANES, blocks - 2)
    line = (row + 4) * groups + chan // SUB
    code = ((line * SUB + chan % SUB) * blocks + blk) * WIDE + col - blk * LANES
    step = rows * groups * SUB * blocks * WIDE
    feats = jnp.concatenate(split3(jnp.concatenate([val[...], wgt[...], iw[...], jnp.zeros((1, held), F32)], 0)), 0)
    pad = jnp.zeros((SUB - 3, held), F32)
    dest = lax.broadcasted_iota(I32, (n, held), 0)
    hit = (tgt == dest) | ((tgt == dest + 1) & (row <= 1)) | ((tgt == dest - 1) & (row >= rows - 3))
    hit = hit & live
    tri = lax.broadcasted_iota(I32, (held, held), 0) < lax.broadcasted_iota(I32, (held, held), 1)
    hit_f = hit.astype(F32)
    rank = jnp.dot(hit_f.astype(BF16), tri.astype(F32).astype(BF16), preferred_element_type=F32)
    place = jnp.where(hit, rank, -1.0)
    total = jnp.sum(hit_f, axis=1, keepdims=True)
    slot = lax.broadcasted_iota(I32, (LANES, held), 0).astype(F32)
    sub8 = lax.broadcasted_iota(I32, (SUB, LANES), 0)
    lane8 = lax.broadcasted_iota(I32, (SUB, LANES), 1)
    least = float(groups * SUB * blocks * WIDE)
    for d in range(n):
        pick = (place[d : d + 1, :] == slot).astype(F32).astype(BF16)
        code_d = (code + (tgt - d) * step).astype(F32)
        lhs = jnp.concatenate([feats, *split3(code_d), pad], 0).astype(BF16)
        got = lax.dot_general(lhs, pick, (((1,), (1,)), ((), ())), preferred_element_type=F32)
        where = jnp.maximum(got[24:25] + got[25:26] + got[26:27], least)
        got = got[0:8] + got[8:16] + got[16:24]
        got = jnp.where(sub8 == 7, where, got)
        msg[d] = jnp.where((sub8 == 7) & (lane8 == LANES - 1), total[d : d + 1, 0:1], got)


class Dense:
    def __init__(self, coef, chans, cols):
        self.coef, self.chans, self.cols = coef, chans, cols
        self.groups, self.blocks = chans // SUB, cols // LANES

    def get(self, ref, x, b):
        v = ref[pl.ds(x * self.groups, self.groups), :, b * LANES : (b + 1) * LANES]
        return v.reshape(self.chans, LANES)

    def row(self, ref, x):
        return [self.get(ref, x, b) for b in range(self.blocks)]

    def put(self, ref, x, b, v):
        at = pl.ds(x * self.groups, self.groups)
        ref[at, :, b * LANES : (b + 1) * LANES] = v.reshape(self.groups, SUB, LANES)

    def mixed(self, lhs, parts):
        res = []
        for b in range(0, self.blocks, 2):
            v = jnp.concatenate(parts[b : b + 2], 1)
            hi = v.astype(BF16).astype(F32)
            rhs = jnp.concatenate([hi, v - hi, hi], 0).astype(BF16)
            r = jnp.dot(lhs, rhs, preferred_element_type=F32)
            res += [r[:, :LANES], r[:, LANES:]]
        return res

    def stencil(self, ref, x, parts, sign):
        coef = self.coef
        lane = lax.broadcasted_iota(I32, (self.chans, LANES), 1)
        zero = jnp.zeros((self.chans, LANES), F32)
        kn, ks, ke, kw = (0, 1, 2, 3) if sign > 0 else (1, 0, 3, 2)
        res = []
        left = [pltpu.roll(v, LANES - 1, 1) for v in parts] + [zero]
        right = [zero] + [pltpu.roll(v, 1, 1) for v in parts]
        for b in range(self.blocks):
            east = jnp.where(lane == LANES - 1, left[b + 1], left[b])
            west = jnp.where(lane == 0, right[b], right[b + 1])
            r = coef[4] * parts[b] + coef[kn] * self.get(ref, x + 1, b) + coef[ks] * self.get(ref, x - 1, b)
            res.append(r + coef[ke] * east + coef[kw] * west)
        return res

    def advance(self, src, x, lhs, dst, slope, y):
        v = self.row(src, x)
        t = [jnp.tanh(p) for p in v]
        p = self.mixed(lhs, t)
        s = self.stencil(src, x, v, 1)
        for b in range(self.blocks):
            self.put(slope, y, b, 1.0 - t[b] * t[b])
            self.put(dst, y, b, s[b] + p[b])


def over(count, bodies):
    def several(i, _):
        for body in bodies:
            body(i)
        return 0

    lax.fori_loop(0, count, several, 0)


def weights(mats, k, chans):
    return mats[k, 0:chans, 0 : 3 * chans].astype(BF16)


def scatter_coefficients(coef, mats, dif, adv, mix, chans, levels):
    for ch in range(chans):
        i, j = ch // levels, ch % levels
        c, a, b = dif[j, i], adv[0, j, i], adv[1, j, i]
        for k, v in enumerate((c + a, c - a, c + b, c - b, 1.0 - 4.0 * c)):
            coef[k, ch : ch + 1, :] = jnp.full((1, LANES), v, F32)
    mats[2] = jnp.zeros((LANES, LANES), F32)
    m = mix[...]
    mats[2, 0:chans, 0:chans] = m
    mt = mats[2].T[0:chans, 0:chans]
    for k, v in enumerate((m, mt)):
        hi = v.astype(BF16).astype(F32)
        mats[k, 0:chans, 0:chans] = hi
        mats[k, 0:chans, chans : 2 * chans] = hi
        mats[k, 0:chans, 2 * chans : 3 * chans] = v - hi


def inner_kernel(
    dif, adv, u_hbm, b_hbm, mix, u1_out, u2_out, dt0_out, dt1_out, base_out, coef, mats,
    u0, base, u1, u2, dt0, dt1, sem_u, sem_b, sem_o, *, rows, cols, chans, levels,
):
    dense = Dense(coef, chans, cols)
    groups = dense.groups
    line = lambda ref, x: ref.at[pl.ds(x * groups, groups)]
    load_u = [pltpu.make_async_copy(u_hbm.at[:, :, x], line(u0, x), sem_u.at[x]) for x in range(rows)]
    load_b = [pltpu.make_async_copy(b_hbm.at[:, :, x], line(base, x), sem_b.at[x]) for x in range(rows)]
    for c in load_u + load_b:
        c.start()
    scatter_coefficients(coef, mats, dif, adv, mix, chans, levels)
    fwd = weights(mats, 0, chans)
    give = lambda ref, out, x, k: pltpu.make_async_copy(line(ref, x), line(out, x), sem_o.at[k, x])
    for c in load_u:
        c.wait()

    def step(off):
        def body(i):
            x = off + i
            dense.advance(u0, x + 1, fwd, u1, dt0, x)
            give(u1, u1_out, x, 0).start()
            give(dt0, dt0_out, x, 1).start()

        return body

    def step2(off):
        def body(i):
            x = off + i
            dense.advance(u1, x + 1, fwd, u2, dt1, x)
            give(u2, u2_out, x, 2).start()
            give(dt1, dt1_out, x, 3).start()

        return body

    half, half2 = (rows - 2) // 2, (rows - 4) // 2
    over(half, [step(0), step(half)])
    over(half2, [step2(0), step2(half2)])
    for c in load_b:
        c.wait()

    def departure(x):
        for b in range(dense.blocks):
            dense.put(base, x, b, dense.get(u0, x, b) - dense.get(base, x, b))
        give(base, base_out, x, 4).start()

    over(rows, [departure])
    for x in range(rows - 2):
        give(u1, u1_out, x, 0).wait()
        give(dt0, dt0_out, x, 1).wait()
    for x in range(rows - 4):
        give(u2, u2_out, x, 2).wait()
        give(dt1, dt1_out, x, 3).wait()
    for x in range(rows):
        give(base, base_out, x, 4).wait()


def main_kernel(
    up_hbm, dn_hbm, msg, u_hbm, u1_in, u2_in, dt0_in, dt1_in, base_in, coef, mats,
    out_hbm, u0, base, u1, u2, f1, f2, dt0, dt1,
    stage, tab, table, code_v, code_s, list_s, sem_e, sem_i, sem_o, sem_m, *, n, rows, cols, chans,
):
    dense = Dense(coef, chans, cols)
    groups, blocks = dense.groups, dense.blocks
    line = lambda ref, x: ref.at[pl.ds(x * groups, groups)]
    store_o = lambda x: pltpu.make_async_copy(line(base, x), out_hbm.at[:, :, x], sem_o.at[x])
    span = HALO * groups
    edges = [
        pltpu.make_async_copy(up_hbm, u0.at[pl.ds(0, span)], sem_e.at[0]),
        pltpu.make_async_copy(dn_hbm, u0.at[pl.ds(span + rows * groups, span)], sem_e.at[1]),
    ]
    for k, x in enumerate((0, 1, rows - 2, rows - 1)):
        edges.append(pltpu.make_async_copy(u_hbm.at[:, :, x], line(u0, HALO + x), sem_e.at[2 + k]))
    bulk = lambda src, ref, x, count, k: pltpu.make_async_copy(
        src, ref.at[pl.ds(x * groups, count * groups)], sem_i.at[k]
    )
    early = [bulk(u1_in, u1, 5, rows - 2, 0), bulk(u2_in, u2, 5, rows - 4, 1)]
    late = [bulk(dt1_in, dt1, 5, rows - 4, 2), bulk(dt0_in, dt0, 5, rows - 2, 3), bulk(base_in, base, 0, rows, 4)]
    for c in edges + early + late:
        c.start()
    code_v[...] = msg[:, SUB - 1, :].astype(I32)
    codes = pltpu.make_async_copy(code_v, code_s, sem_m)
    codes.start()
    fwd, bwd = weights(mats, 0, chans), weights(mats, 1, chans)

    def spread(i):
        for r in range(4):
            s = i * 4 + r
            tab[pl.ds(s * LANES, LANES), 0:SUB] = msg[s].T

    over(n // 4, [spread])
    f1[...] = jnp.zeros_like(f1)
    f2[...] = jnp.zeros_like(f2)
    me = lax.axis_index("gx")
    for c in edges:
        c.wait()

    def clear(ref, x, count):
        ref[pl.ds(x * groups, count * groups)] = jnp.zeros((count * groups, SUB, cols), F32)

    step = lambda off: lambda i: dense.advance(u0, off + 1 + i, fwd, u1, dt0, off + i)
    over(5, [step(0), step(rows + 3)])

    @pl.when(me == 0)
    def _():
        clear(u1, 0, 4)

    @pl.when(me == n - 1)
    def _():
        clear(u1, rows + 4, 4)

    for c in early:
        c.wait()

    step2 = lambda off: lambda i: dense.advance(u1, off + 1 + i, fwd, u2, dt1, off + i)
    over(5, [step2(0), step2(rows + 1)])

    codes.wait()
    unroll = 4
    shift = (WIDE.bit_length() - 1, blocks.bit_length() - 1, SUB.bit_length() - 1)

    def at(code):
        q = lax.shift_right_logical(code, shift[0])
        y = pl.multiple_of(lax.shift_left(q & (blocks - 1), 7), LANES)
        q = lax.shift_right_logical(q, shift[1])
        return lax.shift_right_logical(q, shift[2]), pl.ds(q & (SUB - 1), 1), pl.ds(y, WIDE)

    def gather_src(s, off):
        cnt = code_s[s, LANES - 1]

        def some(i, _):
            for r in range(unroll):
                k = i * unroll + r
                p = off + k
                code = code_s[s, k]
                list_s[p] = code
                x, at_s, at_y = at(code)
                at_p = pl.ds(p, 1)
                stage[0, at_p] = u1[x, at_s, at_y]
                stage[1, at_p] = u1[x + groups, at_s, at_y]
                stage[2, at_p] = u2[x - groups, at_s, at_y]
                stage[3, at_p] = u2[x, at_s, at_y]
                table[at_p] = tab[pl.ds(s * LANES + k, 1)]
            return 0

        lax.fori_loop(0, lax.shift_right_logical(cnt + unroll - 1, 2), some, 0)
        return off + cnt

    count = lax.fori_loop(0, n, gather_src, 0)
    for r in range(unroll):
        list_s[count + r] = groups * SUB * blocks * WIDE

    per = 64
    lane1 = lax.broadcasted_iota(I32, (per, LANES), 1)
    nth = lax.broadcasted_iota(I32, (per, LANES), 0)

    def misfits(g, _):
        p = pl.multiple_of(g * per, per)
        at_p = pl.ds(p, per)
        rec = table[at_p]
        wide = lambda k: jnp.broadcast_to(rec[:, k : k + 1], (per, LANES))
        l = wide(7).astype(I32) & (WIDE - 1)
        iw = [wide(k) for k in range(3, 7)]
        ws = []
        for h in range(2):
            here, nxt = lane1 == l - h * LANES, lane1 == l + (1 - h * LANES)
            ws.append([jnp.where(here, iw[k], jnp.where(nxt, iw[k + 1], 0.0)) for k in (0, 2)])
        w = jnp.where(p + nth < count, wide(2), 0.0)
        for t in range(2):
            q = 0.0
            for k in range(2):
                for h in range(2):
                    q = q + ws[h][k] * stage[2 * t + k, at_p, h * LANES : (h + 1) * LANES]
            d = jnp.broadcast_to(jnp.sum(q, 1, keepdims=True), (per, LANES)) - wide(t)
            d = jnp.where(w > 0.0, w * d, 0.0)
            for k in range(2):
                for h in range(2):
                    stage[2 * t + k, at_p, h * LANES : (h + 1) * LANES] = d * ws[h][k]
        return 0

    lax.fori_loop(0, lax.div(count + per - 1, per), misfits, 0)

    def scatter(i, _):
        for r in range(unroll):
            p = i * unroll + r
            x, at_s, at_y = at(list_s[p])
            at_p = pl.ds(p, 1)
            a = f1[x - groups, at_s, at_y] + stage[0, at_p]
            b = f1[x, at_s, at_y] + stage[1, at_p]
            c = f2[x - groups, at_s, at_y] + stage[2, at_p]
            d = f2[x, at_s, at_y] + stage[3, at_p]
            f1[x - groups, at_s, at_y] = a
            f1[x, at_s, at_y] = b
            f2[x - groups, at_s, at_y] = c
            f2[x, at_s, at_y] = d
        return 0

    lax.fori_loop(0, lax.shift_right_logical(count + unroll - 1, 2), scatter, 0)

    def third(off):
        def body(i):
            k = off + i
            v = dense.row(f2, k)
            p = dense.mixed(bwd, v)
            s = dense.stencil(f2, k, v, -1)
            for b in range(blocks):
                dense.put(f1, k, b, (s[b] + dense.get(f1, k, b)) + dense.get(dt1, k, b) * p[b])

        return body

    for c in late:
        c.wait()
    half = (rows + 2) // 2
    over(half, [third(2), third(2 + half)])

    @pl.when(me == 0)
    def _():
        clear(f1, 2, 1)

    @pl.when(me == n - 1)
    def _():
        clear(f1, rows + 3, 1)

    def fourth(off):
        def body(i):
            x = off + i
            k = x + 3
            v = dense.row(f1, k)
            p = dense.mixed(bwd, v)
            s = dense.stencil(f1, k, v, -1)
            for b in range(blocks):
                r = s[b] + dense.get(dt0, x + 4, b) * p[b]
                dense.put(base, x, b, dense.get(base, x, b) + r)
            store_o(x).start()

        return body

    over(rows // 2, [fourth(0), fourth(rows // 2)])
    for x in range(rows):
        store_o(x).wait()


def shards(
    initial, background, mixing, diffusion, advection, obs_values, obs_weight, interp_weights,
    stencil_index, station_tile, counts,
):
    fields, levels, rows, cols = initial.shape
    chans = fields * levels
    groups = chans // SUB
    n = lax.axis_size("gx")
    held = obs_values.shape[1]
    cap = max(2, held * 3 // (2 * n))
    most = -(-3 * cap * n // 64) * 64 + 64
    in_hbm = lambda x: pltpu.with_memory_space_constraint(x, pltpu.HBM)
    u = in_hbm(initial.reshape(groups, SUB, rows, cols))
    b = in_hbm(background.reshape(groups, SUB, rows, cols))
    vmem, smem, hbm = (pl.BlockSpec(memory_space=s) for s in (pltpu.VMEM, pltpu.SMEM, pltpu.HBM))
    anywhere = pl.BlockSpec(memory_space=pl.ANY)
    buf = lambda count: pltpu.VMEM((count * groups, SUB, cols), F32)
    shape = lambda count: jax.ShapeDtypeStruct((count * groups, SUB, cols), F32)
    up_send, dn_send = pl.pallas_call(
        functools.partial(edges_kernel, rows=rows, groups=groups),
        out_shape=(shape(HALO), shape(HALO)),
        in_specs=[hbm],
        out_specs=(vmem, vmem),
        scratch_shapes=[pltpu.SemaphoreType.DMA((2 * HALO,))],
        compiler_params=pltpu.CompilerParams(vmem_limit_bytes=16 << 20),
        name="edges",
    )(u)
    up = [(i, i + 1) for i in range(n - 1)]
    down = [(j, i) for i, j in up]
    from_up = lax.ppermute(up_send, "gx", up)
    from_dn = lax.ppermute(dn_send, "gx", down)
    msg = pl.pallas_call(
        functools.partial(bucket_kernel, n=n, rows=rows, cols=cols, groups=groups),
        out_shape=jax.ShapeDtypeStruct((n, SUB, LANES), F32),
        in_specs=[vmem, vmem, vmem, vmem, vmem, smem],
        out_specs=vmem,
        compiler_params=pltpu.CompilerParams(vmem_limit_bytes=16 << 20),
        name="bucket",
    )(obs_values, obs_weight, interp_weights, stencil_index, station_tile.T, counts)
    msg = lax.all_to_all(msg, "gx", split_axis=0, concat_axis=0, tiled=True)
    dma = pltpu.SemaphoreType.DMA
    ready = pl.pallas_call(
        functools.partial(inner_kernel, rows=rows, cols=cols, chans=chans, levels=levels),
        out_shape=(
            *[pltpu.HBM(((rows - k) * groups, SUB, cols), F32) for k in (2, 4, 2, 4, 0)],
            jax.ShapeDtypeStruct((5, chans, LANES), F32),
            jax.ShapeDtypeStruct((3, LANES, LANES), F32),
        ),
        in_specs=[smem, smem, hbm, hbm, vmem],
        out_specs=(*[hbm] * 5, vmem, vmem),
        scratch_shapes=[buf(rows - k) for k in (0, 0, 2, 4, 2, 4)]
        + [dma((rows,)), dma((rows,)), dma((5, rows))],
        compiler_params=pltpu.CompilerParams(vmem_limit_bytes=24 << 20),
        name="inner",
    )(diffusion.T, advection.transpose(0, 2, 1), u, b, mixing)
    out = pl.pallas_call(
        functools.partial(main_kernel, n=n, rows=rows, cols=cols, chans=chans),
        out_shape=jax.ShapeDtypeStruct(u.shape, F32),
        in_specs=[anywhere, anywhere, vmem, *[hbm] * 6, vmem, vmem],
        out_specs=hbm,
        scratch_shapes=[buf(rows + k) for k in (2 * HALO, 0, 8, 6, 6, 6, 8, 6)]
        + [
            pltpu.VMEM((4, most, WIDE), F32),
            pltpu.VMEM((n * LANES, LANES), F32),
            pltpu.VMEM((most, LANES), F32),
            pltpu.VMEM((n, LANES), I32),
            pltpu.SMEM((n, LANES), I32),
            pltpu.SMEM((most,), I32),
            dma((6,)),
            dma((5,)),
            dma((rows,)),
            dma(()),
        ],
        compiler_params=pltpu.CompilerParams(vmem_limit_bytes=48 << 20),
        name="adjoint",
    )(from_up, from_dn, msg, u, *map(in_hbm, ready[:5]), *ready[5:])
    return out.reshape(fields, levels, rows, cols)


def solution(mesh):
    placed = (
        P("groups", None, "gx", None),
        P("groups", None, "gx", None),
        P(),
        P(),
        P(),
        P("groups", "gx"),
        P("groups", "gx"),
        P("groups", "gx"),
        P("groups", "gx"),
        P("gx", "groups"),
        P("groups", "gx"),
    )
    return jax.shard_map(
        shards, mesh=mesh, in_specs=placed, out_specs=P("groups", None, "gx", None), check_vma=False
    )
```

```python
import functools

import jax
import jax.numpy as jnp
from jax import lax
from jax.experimental import pallas as pl
from jax.experimental.pallas import tpu as pltpu
from jax.sharding import PartitionSpec as P

HALO = 5
LANES = 128
WIDE = 2 * LANES
SUB = 8
F32, BF16, I32 = jnp.float32, jnp.bfloat16, jnp.int32


def split3(x):
    hi = x.astype(BF16).astype(F32)
    mid = (x - hi).astype(BF16).astype(F32)
    return [hi, mid, x - hi - mid]


def edges_kernel(u_hbm, odd, even, sem, *, rows, groups):
    parity = lax.axis_index("gx") & 1
    last = rows - HALO
    copies = []
    for k in range(HALO):
        at = pl.ds(k * groups, groups)
        copies.append(pltpu.make_async_copy(u_hbm.at[:, :, parity * last + k], odd.at[at], sem.at[k]))
        copies.append(pltpu.make_async_copy(u_hbm.at[:, :, (1 - parity) * last + k], even.at[at], sem.at[HALO + k]))
    for c in copies:
        c.start()
    for c in copies:
        c.wait()


def bucket_kernel(val, wgt, iw, cell, tile, cnt, msg, *, n, rows, cols, groups):
    held = val.shape[1]
    blocks = cols // LANES
    tgt = tile[...]
    lane = lax.broadcasted_iota(I32, (1, held), 1)
    live = lane < cnt[0, 0]
    base = cell[0:1, :]
    plane = rows * cols
    chan = base // plane
    rest = base - chan * plane
    row = rest // cols
    col = rest - row * cols
    blk = jnp.minimum(col // LANES, blocks - 2)
    line = (row + 4) * groups + chan // SUB
    code = ((line * SUB + chan % SUB) * blocks + blk) * WIDE + col - blk * LANES
    step = rows * groups * SUB * blocks * WIDE
    feats = jnp.concatenate(split3(jnp.concatenate([val[...], wgt[...], iw[...], jnp.zeros((1, held), F32)], 0)), 0)
    pad = jnp.zeros((SUB - 3, held), F32)
    dest = lax.broadcasted_iota(I32, (n, held), 0)
    hit = (tgt == dest) | ((tgt == dest + 1) & (row <= 1)) | ((tgt == dest - 1) & (row >= rows - 3))
    hit = hit & live
    tri = lax.broadcasted_iota(I32, (held, held), 0) < lax.broadcasted_iota(I32, (held, held), 1)
    hit_f = hit.astype(F32)
    rank = jnp.dot(hit_f.astype(BF16), tri.astype(F32).astype(BF16), preferred_element_type=F32)
    place = jnp.where(hit, rank, -1.0)
    total = jnp.sum(hit_f, axis=1, keepdims=True)
    slot = lax.broadcasted_iota(I32, (LANES, held), 0).astype(F32)
    sub8 = lax.broadcasted_iota(I32, (SUB, LANES), 0)
    lane8 = lax.broadcasted_iota(I32, (SUB, LANES), 1)
    least = float(groups * SUB * blocks * WIDE)
    for d in range(n):
        pick = (place[d : d + 1, :] == slot).astype(F32).astype(BF16)
        code_d = (code + (tgt - d) * step).astype(F32)
        lhs = jnp.concatenate([feats, *split3(code_d), pad], 0).astype(BF16)
        got = lax.dot_general(lhs, pick, (((1,), (1,)), ((), ())), preferred_element_type=F32)
        where = jnp.maximum(got[24:25] + got[25:26] + got[26:27], least)
        got = got[0:8] + got[8:16] + got[16:24]
        got = jnp.where(sub8 == 7, where, got)
        msg[d] = jnp.where((sub8 == 7) & (lane8 == LANES - 1), total[d : d + 1, 0:1], got)


class Dense:
    def __init__(self, coef, chans, cols):
        self.coef, self.chans, self.cols = coef, chans, cols
        self.groups, self.blocks = chans // SUB, cols // LANES

    def get(self, ref, x, b):
        v = ref[pl.ds(x * self.groups, self.groups), :, b * LANES : (b + 1) * LANES]
        return v.reshape(self.chans, LANES)

    def row(self, ref, x):
        return [self.get(ref, x, b) for b in range(self.blocks)]

    def put(self, ref, x, b, v):
        at = pl.ds(x * self.groups, self.groups)
        ref[at, :, b * LANES : (b + 1) * LANES] = v.reshape(self.groups, SUB, LANES)

    def mixed(self, lhs, parts):
        res = []
        for b in range(0, self.blocks, 2):
            v = jnp.concatenate(parts[b : b + 2], 1)
            hi = v.astype(BF16).astype(F32)
            rhs = jnp.concatenate([hi, v - hi, hi], 0).astype(BF16)
            r = jnp.dot(lhs, rhs, preferred_element_type=F32)
            res += [r[:, :LANES], r[:, LANES:]]
        return res

    def stencil(self, ref, x, parts, sign):
        coef = self.coef
        lane = lax.broadcasted_iota(I32, (self.chans, LANES), 1)
        zero = jnp.zeros((self.chans, LANES), F32)
        kn, ks, ke, kw = (0, 1, 2, 3) if sign > 0 else (1, 0, 3, 2)
        res = []
        left = [pltpu.roll(v, LANES - 1, 1) for v in parts] + [zero]
        right = [zero] + [pltpu.roll(v, 1, 1) for v in parts]
        for b in range(self.blocks):
            east = jnp.where(lane == LANES - 1, left[b + 1], left[b])
            west = jnp.where(lane == 0, right[b], right[b + 1])
            r = coef[4] * parts[b] + coef[kn] * self.get(ref, x + 1, b) + coef[ks] * self.get(ref, x - 1, b)
            res.append(r + coef[ke] * east + coef[kw] * west)
        return res

    def advance(self, src, x, lhs, dst, slope, y):
        v = self.row(src, x)
        t = [jnp.tanh(p) for p in v]
        p = self.mixed(lhs, t)
        s = self.stencil(src, x, v, 1)
        for b in range(self.blocks):
            self.put(slope, y, b, 1.0 - t[b] * t[b])
            self.put(dst, y, b, s[b] + p[b])


def over(count, bodies, after=None):
    def several(i, _):
        for body in bodies:
            body(i)
        if after is not None:
            after(i)
        return 0

    lax.fori_loop(0, count, several, 0)


def weights(mats, k, chans):
    return mats[k, 0:chans, 0 : 3 * chans].astype(BF16)


def scatter_coefficients(coef, mats, dif, adv, mix, chans, levels):
    for ch in range(chans):
        i, j = ch // levels, ch % levels
        c, a, b = dif[j, i], adv[0, j, i], adv[1, j, i]
        for k, v in enumerate((c + a, c - a, c + b, c - b, 1.0 - 4.0 * c)):
            coef[k, ch : ch + 1, :] = jnp.full((1, LANES), v, F32)
    mats[2] = jnp.zeros((LANES, LANES), F32)
    m = mix[...]
    mats[2, 0:chans, 0:chans] = m
    mt = mats[2].T[0:chans, 0:chans]
    for k, v in enumerate((m, mt)):
        hi = v.astype(BF16).astype(F32)
        mats[k, 0:chans, 0:chans] = hi
        mats[k, 0:chans, chans : 2 * chans] = hi
        mats[k, 0:chans, 2 * chans : 3 * chans] = v - hi


def inner_kernel(
    dif, adv, u_hbm, b_hbm, mix, u1_out, u2_out, dt0_out, dt1_out, base_out, coef, mats,
    u0, base, u1, u2, dt0, dt1, sem_u, sem_b, sem_o, *, rows, cols, chans, levels,
):
    dense = Dense(coef, chans, cols)
    groups = dense.groups
    line = lambda ref, x: ref.at[pl.ds(x * groups, groups)]
    load_u = [pltpu.make_async_copy(u_hbm.at[:, :, x], line(u0, x), sem_u.at[x]) for x in range(rows)]
    load_b = [pltpu.make_async_copy(b_hbm.at[:, :, x], line(base, x), sem_b.at[x]) for x in range(rows)]
    for c in load_u + load_b:
        c.start()
    scatter_coefficients(coef, mats, dif, adv, mix, chans, levels)
    fwd = weights(mats, 0, chans)
    give = lambda ref, out, x, k: pltpu.make_async_copy(line(ref, x), line(out, x), sem_o.at[k, x])
    for c in load_u:
        c.wait()

    half, half2 = (rows - 2) // 2, (rows - 4) // 2
    step = lambda off: lambda i: dense.advance(u0, off + i + 1, fwd, u1, dt0, off + i)
    step2 = lambda off: lambda i: dense.advance(u1, off + i + 1, fwd, u2, dt1, off + i)

    def give1(i):
        for x in (i, half + i):
            give(u1, u1_out, x, 0).start()
            give(dt0, dt0_out, x, 1).start()

    def give2(i):
        for x in (i, half2 + i):
            give(u2, u2_out, x, 2).start()
            give(dt1, dt1_out, x, 3).start()

    over(half, [step(0), step(half)], give1)
    over(half2, [step2(0), step2(half2)], give2)
    for c in load_b:
        c.wait()

    def departure(x):
        for b in range(dense.blocks):
            dense.put(base, x, b, dense.get(u0, x, b) - dense.get(base, x, b))
        give(base, base_out, x, 4).start()

    over(rows, [departure])
    for x in range(rows - 2):
        give(u1, u1_out, x, 0).wait()
        give(dt0, dt0_out, x, 1).wait()
    for x in range(rows - 4):
        give(u2, u2_out, x, 2).wait()
        give(dt1, dt1_out, x, 3).wait()
    for x in range(rows):
        give(base, base_out, x, 4).wait()


def main_kernel(
    odd_hbm, even_hbm, msg, u_hbm, u1_in, u2_in, dt0_in, dt1_in, base_in, coef, mats,
    out_hbm, u0, base, u1, u2, f1, f2, dt0, dt1,
    stage, table, code_v, code_s, list_v, list_s, sem_e, sem_i, sem_o, sem_m, sem_l,
    *, n, rows, cols, chans, slots,
):
    dense = Dense(coef, chans, cols)
    groups, blocks = dense.groups, dense.blocks
    line = lambda ref, x: ref.at[pl.ds(x * groups, groups)]
    store_o = lambda x: pltpu.make_async_copy(line(base, x), out_hbm.at[:, :, x], sem_o.at[x])
    span = HALO * groups
    me = lax.axis_index("gx")
    below = span + rows * groups
    edges = [
        pltpu.make_async_copy(odd_hbm, u0.at[pl.ds((me & 1) * below, span)], sem_e.at[0]),
        pltpu.make_async_copy(even_hbm, u0.at[pl.ds((1 - (me & 1)) * below, span)], sem_e.at[1]),
    ]
    for k, x in enumerate((0, 1, rows - 2, rows - 1)):
        edges.append(pltpu.make_async_copy(u_hbm.at[:, :, x], line(u0, HALO + x), sem_e.at[2 + k]))
    bulk = lambda src, ref, x, count, k: pltpu.make_async_copy(
        src, ref.at[pl.ds(x * groups, count * groups)], sem_i.at[k]
    )
    early = [bulk(u1_in, u1, 5, rows - 2, 0), bulk(u2_in, u2, 5, rows - 4, 1)]
    late = [bulk(dt1_in, dt1, 5, rows - 4, 2), bulk(dt0_in, dt0, 5, rows - 2, 3), bulk(base_in, base, 0, rows, 4)]
    for c in edges + early + late:
        c.start()
    code_v[...] = msg[:, SUB - 1, :].astype(I32)
    codes = pltpu.make_async_copy(code_v, code_s, sem_m)
    codes.start()
    fwd, bwd = weights(mats, 0, chans), weights(mats, 1, chans)

    f1[...] = jnp.zeros_like(f1)
    f2[...] = jnp.zeros_like(f2)

    codes.wait()

    def compact(s, off):
        table[pl.ds(off, slots), 0:SUB] = msg[s].T[0:slots]
        return off + code_s[s, LANES - 1]

    count = lax.fori_loop(0, n, compact, 0)
    lane_at = lax.broadcasted_iota(I32, (1, LANES), 1)
    safe = groups * SUB * blocks * WIDE

    def enlist(q, _):
        at = pl.multiple_of(q * LANES, LANES)
        code = table[pl.ds(at, LANES), :].T[SUB - 1 : SUB].astype(I32)
        list_v[pl.ds(q, 1)] = jnp.where(at + lane_at < count, code, safe)
        return 0

    lax.fori_loop(0, lax.shift_right_logical(count + LANES - 1, 7), enlist, 0)
    lists = pltpu.make_async_copy(list_v, list_s, sem_l)
    lists.start()
    for c in edges:
        c.wait()

    def clear(ref, x, count):
        ref[pl.ds(x * groups, count * groups)] = jnp.zeros((count * groups, SUB, cols), F32)

    step = lambda off: lambda i: dense.advance(u0, off + 1 + i, fwd, u1, dt0, off + i)
    over(5, [step(0), step(rows + 3)])

    @pl.when(me == 0)
    def _():
        clear(u1, 0, 4)

    @pl.when(me == n - 1)
    def _():
        clear(u1, rows + 4, 4)

    for c in early:
        c.wait()

    step2 = lambda off: lambda i: dense.advance(u1, off + 1 + i, fwd, u2, dt1, off + i)
    over(5, [step2(0), step2(rows + 1)])

    lists.wait()
    shift = (WIDE.bit_length() - 1, blocks.bit_length() - 1, SUB.bit_length() - 1)

    def at(code):
        q = lax.shift_right_logical(code, shift[0])
        y = pl.multiple_of(lax.shift_left(q & (blocks - 1), 7), LANES)
        q = lax.shift_right_logical(q, shift[1])
        return lax.shift_right_logical(q, shift[2]), pl.ds(q & (SUB - 1), 1), pl.ds(y, WIDE)

    def entry(i, r):
        return at(list_s[lax.shift_right_logical(i, 4), lax.shift_left(i & 15, 3) + r])

    def gather(i, _):
        for r in range(SUB):
            x, at_s, at_y = entry(i, r)
            stage[0, i, r : r + 1] = u1[x, at_s, at_y]
            stage[1, i, r : r + 1] = u1[x + groups, at_s, at_y]
            stage[2, i, r : r + 1] = u2[x - groups, at_s, at_y]
            stage[3, i, r : r + 1] = u2[x, at_s, at_y]
        return 0

    turns = lax.shift_right_logical(count + SUB - 1, 3)
    lax.fori_loop(0, turns, gather, 0)

    per = 64
    lane1 = lax.broadcasted_iota(I32, (per, LANES), 1)
    nth = lax.broadcasted_iota(I32, (per, LANES), 0)

    def misfits(g, _):
        p = pl.multiple_of(g * per, per)
        at_p = pl.ds(pl.multiple_of(g * (per // SUB), per // SUB), per // SUB)
        rec = table[pl.ds(p, per)]
        wide = lambda k: jnp.broadcast_to(rec[:, k : k + 1], (per, LANES))
        valid = p + nth < count
        l = jnp.where(valid, wide(7).astype(I32) & (WIDE - 1), -WIDE)
        iw = [wide(k) for k in range(3, 7)]
        ws = []
        for h in range(2):
            here, nxt = lane1 == l - h * LANES, lane1 == l + (1 - h * LANES)
            ws.append([jnp.where(here, iw[k], jnp.where(nxt, iw[k + 1], 0.0)) for k in (0, 2)])
        w = wide(2)
        cut = lambda h: slice(h * LANES, (h + 1) * LANES)
        for t in range(2):
            q = 0.0
            for k in range(2):
                for h in range(2):
                    q = q + ws[h][k] * stage[2 * t + k, at_p, :, cut(h)].reshape(per, LANES)
            d = jnp.broadcast_to(jnp.sum(q, 1, keepdims=True), (per, LANES)) - wide(t)
            d = jnp.where(valid, w * d, 0.0)
            for k in range(2):
                for h in range(2):
                    stage[2 * t + k, at_p, :, cut(h)] = (d * ws[h][k]).reshape(per // SUB, SUB, LANES)
        return 0

    lax.fori_loop(0, lax.shift_right_logical(count + per - 1, 6), misfits, 0)

    def scatter(i, _):
        for r in range(SUB):
            x, at_s, at_y = entry(i, r)
            a = f1[x - groups, at_s, at_y] + stage[0, i, r : r + 1]
            b = f1[x, at_s, at_y] + stage[1, i, r : r + 1]
            c = f2[x - groups, at_s, at_y] + stage[2, i, r : r + 1]
            d = f2[x, at_s, at_y] + stage[3, i, r : r + 1]
            f1[x - groups, at_s, at_y] = a
            f1[x, at_s, at_y] = b
            f2[x - groups, at_s, at_y] = c
            f2[x, at_s, at_y] = d
        return 0

    lax.fori_loop(0, turns, scatter, 0)

    def third(off):
        def body(i):
            k = off + i
            v = dense.row(f2, k)
            p = dense.mixed(bwd, v)
            s = dense.stencil(f2, k, v, -1)
            for b in range(blocks):
                dense.put(f1, k, b, (s[b] + dense.get(f1, k, b)) + dense.get(dt1, k, b) * p[b])

        return body

    for c in late:
        c.wait()
    half = (rows + 2) // 2
    over(half, [third(2), third(2 + half)])

    @pl.when(me == 0)
    def _():
        clear(f1, 2, 1)

    @pl.when(me == n - 1)
    def _():
        clear(f1, rows + 3, 1)

    def fourth(off):
        def body(i):
            x = off + i
            k = x + 3
            v = dense.row(f1, k)
            p = dense.mixed(bwd, v)
            s = dense.stencil(f1, k, v, -1)
            for b in range(blocks):
                r = s[b] + dense.get(dt0, x + 4, b) * p[b]
                dense.put(base, x, b, dense.get(base, x, b) + r)

        return body

    def store2(i):
        store_o(i).start()
        store_o(rows // 2 + i).start()

    over(rows // 2, [fourth(0), fourth(rows // 2)], store2)
    for x in range(rows):
        store_o(x).wait()


def shards(
    initial, background, mixing, diffusion, advection, obs_values, obs_weight, interp_weights,
    stencil_index, station_tile, counts,
):
    fields, levels, rows, cols = initial.shape
    chans = fields * levels
    groups = chans // SUB
    n = lax.axis_size("gx")
    held = obs_values.shape[1]
    cap = max(2, held * 3 // (2 * n))
    slots = -(-3 * cap // SUB) * SUB
    most = -(-(3 * cap * n + slots) // LANES) * LANES
    in_hbm = lambda x: pltpu.with_memory_space_constraint(x, pltpu.HBM)
    u = in_hbm(initial.reshape(groups, SUB, rows, cols))
    b = in_hbm(background.reshape(groups, SUB, rows, cols))
    vmem, smem, hbm = (pl.BlockSpec(memory_space=s) for s in (pltpu.VMEM, pltpu.SMEM, pltpu.HBM))
    anywhere = pl.BlockSpec(memory_space=pl.ANY)
    buf = lambda count: pltpu.VMEM((count * groups, SUB, cols), F32)
    shape = lambda count: jax.ShapeDtypeStruct((count * groups, SUB, cols), F32)
    odd_send, even_send = pl.pallas_call(
        functools.partial(edges_kernel, rows=rows, groups=groups),
        out_shape=(buf(HALO), buf(HALO)),
        in_specs=[hbm],
        out_specs=(vmem, vmem),
        scratch_shapes=[pltpu.SemaphoreType.DMA((2 * HALO,))],
        compiler_params=pltpu.CompilerParams(vmem_limit_bytes=16 << 20),
        name="edges",
    )(u)
    swap = lambda first: [p for i in range(first, n - 1, 2) for p in ((i, i + 1), (i + 1, i))]
    odd = lax.ppermute(odd_send, "gx", swap(1))
    even = lax.ppermute(even_send, "gx", swap(0))
    msg = pl.pallas_call(
        functools.partial(bucket_kernel, n=n, rows=rows, cols=cols, groups=groups),
        out_shape=jax.ShapeDtypeStruct((n, SUB, LANES), F32),
        in_specs=[vmem, vmem, vmem, vmem, vmem, smem],
        out_specs=vmem,
        compiler_params=pltpu.CompilerParams(vmem_limit_bytes=16 << 20),
        name="bucket",
    )(obs_values, obs_weight, interp_weights, stencil_index, station_tile.T, counts)
    msg = lax.all_to_all(msg, "gx", split_axis=0, concat_axis=0, tiled=True)
    dma = pltpu.SemaphoreType.DMA
    ready = pl.pallas_call(
        functools.partial(inner_kernel, rows=rows, cols=cols, chans=chans, levels=levels),
        out_shape=(
            *[pltpu.HBM(((rows - k) * groups, SUB, cols), F32) for k in (2, 4, 2, 4, 0)],
            jax.ShapeDtypeStruct((5, chans, LANES), F32),
            jax.ShapeDtypeStruct((3, LANES, LANES), F32),
        ),
        in_specs=[smem, smem, hbm, hbm, vmem],
        out_specs=(*[hbm] * 5, vmem, vmem),
        scratch_shapes=[buf(rows - k) for k in (0, 0, 2, 4, 2, 4)]
        + [dma((rows,)), dma((rows,)), dma((5, rows))],
        compiler_params=pltpu.CompilerParams(vmem_limit_bytes=24 << 20),
        name="inner",
    )(diffusion.T, advection.transpose(0, 2, 1), u, b, mixing)
    out = pl.pallas_call(
        functools.partial(main_kernel, n=n, rows=rows, cols=cols, chans=chans, slots=slots),
        out_shape=jax.ShapeDtypeStruct(u.shape, F32),
        in_specs=[anywhere, anywhere, vmem, *[hbm] * 6, vmem, vmem],
        out_specs=hbm,
        scratch_shapes=[buf(rows + k) for k in (2 * HALO, 0, 8, 6, 6, 6, 8, 6)]
        + [
            pltpu.VMEM((4, most // SUB, SUB, WIDE), F32),
            pltpu.VMEM((most, LANES), F32),
            pltpu.VMEM((n, LANES), I32),
            pltpu.SMEM((n, LANES), I32),
            pltpu.VMEM((most // LANES, LANES), I32),
            pltpu.SMEM((most // LANES, LANES), I32),
            dma((6,)),
            dma((5,)),
            dma((rows,)),
            dma(()),
            dma(()),
        ],
        compiler_params=pltpu.CompilerParams(vmem_limit_bytes=48 << 20),
        name="adjoint",
    )(odd, even, msg, u, *map(in_hbm, ready[:5]), *ready[5:])
    return out.reshape(fields, levels, rows, cols)


def solution(mesh):
    placed = (
        P("groups", None, "gx", None),
        P("groups", None, "gx", None),
        P(),
        P(),
        P(),
        P("groups", "gx"),
        P("groups", "gx"),
        P("groups", "gx"),
        P("groups", "gx"),
        P("gx", "groups"),
        P("groups", "gx"),
    )
    return jax.shard_map(
        shards, mesh=mesh, in_specs=placed, out_specs=P("groups", None, "gx", None), check_vma=False
    )
```

```python
import functools

import jax
import jax.numpy as jnp
from jax import lax
from jax.experimental import pallas as pl
from jax.experimental.pallas import tpu as pltpu
from jax.sharding import PartitionSpec as P

HALO = 5
NEAR = 2
LANES = 128
WIDE = 2 * LANES
SUB = 8
F32, BF16, I32 = jnp.float32, jnp.bfloat16, jnp.int32


def split3(x):
    hi = x.astype(BF16).astype(F32)
    mid = (x - hi).astype(BF16).astype(F32)
    return [hi, mid, x - hi - mid]


def prep_kernel(u_hbm, val, wgt, iw, cell, tile, cnt, near, far, even, msg, sem, *, n, rows, cols, groups, edge):
    parity = lax.axis_index("gx") & 1
    last = rows - HALO
    copies = []
    start = (parity * (rows - NEAR), parity * last + (1 - parity) * NEAR, (1 - parity) * last)
    for ref, x, count in zip((near, far, even), start, (NEAR, HALO - NEAR, HALO)):
        for k in range(count):
            at = ref.at[pl.ds(k * groups, groups)]
            copies.append(pltpu.make_async_copy(u_hbm.at[:, :, x + k], at, sem.at[len(copies)]))
    for c in copies:
        c.start()
    held = val.shape[1]
    blocks = cols // LANES
    tgt = tile[...]
    lane = lax.broadcasted_iota(I32, (1, held), 1)
    live = lane < cnt[0, 0]
    base = cell[0:1, :]
    plane = rows * cols
    chan = base // plane
    rest = base - chan * plane
    row = rest // cols
    col = rest - row * cols
    blk = jnp.minimum(col // LANES, blocks - 2)
    line = (row + 4) * groups + chan // SUB
    code = ((line * SUB + chan % SUB) * blocks + blk) * WIDE + col - blk * LANES
    step = rows * groups * SUB * blocks * WIDE
    feats = jnp.concatenate(split3(jnp.concatenate([val[...], wgt[...], iw[...], jnp.zeros((1, held), F32)], 0)), 0)
    pad = jnp.zeros((SUB - 3, held), F32)
    dest = lax.broadcasted_iota(I32, (n, held), 0)
    low, high = row <= 1, row >= rows - 3
    own = (tgt == dest) & live
    near = live & ((tgt == dest + 1) & low | (tgt == dest - 1) & high)
    outer = near | own & (low | high)
    within = own & (row >= 2) & (row <= rows - 4)
    hits = jnp.concatenate([within.astype(F32), outer.astype(F32)], 0)
    tri = lax.broadcasted_iota(I32, (held, held), 0) < lax.broadcasted_iota(I32, (held, held), 1)
    rank = jnp.dot(hits.astype(BF16), tri.astype(F32).astype(BF16), preferred_element_type=F32)
    place = jnp.where(within, rank[0:n], jnp.where(outer, rank[n:] + float(edge), -1.0))
    total = jnp.sum(hits, axis=1, keepdims=True)
    slot = lax.broadcasted_iota(I32, (LANES, held), 0).astype(F32)
    sub8 = lax.broadcasted_iota(I32, (SUB, LANES), 0)
    lane8 = lax.broadcasted_iota(I32, (SUB, LANES), 1)
    for d in range(n):
        pick = (place[d : d + 1, :] == slot).astype(F32).astype(BF16)
        code_d = (code + (tgt - d) * step).astype(F32)
        lhs = jnp.concatenate([feats, *split3(code_d), pad], 0).astype(BF16)
        got = lax.dot_general(lhs, pick, (((1,), (1,)), ((), ())), preferred_element_type=F32)
        where = got[24:25] + got[25:26] + got[26:27]
        got = got[0:8] + got[8:16] + got[16:24]
        got = jnp.where(sub8 == 7, where, got)
        got = jnp.where((sub8 == 7) & (lane8 == LANES - 1), total[d : d + 1, 0:1], got)
        msg[d] = jnp.where((sub8 == 7) & (lane8 == LANES - 2), total[n + d : n + d + 1, 0:1], got)
    for c in copies:
        c.wait()


class Dense:
    def __init__(self, coef, chans, cols):
        self.coef, self.chans, self.cols = coef, chans, cols
        self.groups, self.blocks = chans // SUB, cols // LANES

    def get(self, ref, x, b):
        v = ref[pl.ds(x * self.groups, self.groups), :, b * LANES : (b + 1) * LANES]
        return v.reshape(self.chans, LANES)

    def row(self, ref, x):
        return [self.get(ref, x, b) for b in range(self.blocks)]

    def put(self, ref, x, b, v):
        at = pl.ds(x * self.groups, self.groups)
        ref[at, :, b * LANES : (b + 1) * LANES] = v.reshape(self.groups, SUB, LANES)

    def mixed(self, lhs, parts):
        res = []
        for b in range(0, self.blocks, 2):
            v = jnp.concatenate(parts[b : b + 2], 1)
            hi = v.astype(BF16).astype(F32)
            rhs = jnp.concatenate([hi, v - hi, hi], 0).astype(BF16)
            r = jnp.dot(lhs, rhs, preferred_element_type=F32)
            res += [r[:, :LANES], r[:, LANES:]]
        return res

    def stencil(self, ref, x, parts, sign):
        coef = self.coef
        lane = lax.broadcasted_iota(I32, (self.chans, LANES), 1)
        zero = jnp.zeros((self.chans, LANES), F32)
        kn, ks, ke, kw = (0, 1, 2, 3) if sign > 0 else (1, 0, 3, 2)
        res = []
        left = [pltpu.roll(v, LANES - 1, 1) for v in parts] + [zero]
        right = [zero] + [pltpu.roll(v, 1, 1) for v in parts]
        for b in range(self.blocks):
            east = jnp.where(lane == LANES - 1, left[b + 1], left[b])
            west = jnp.where(lane == 0, right[b], right[b + 1])
            r = coef[4] * parts[b] + coef[kn] * self.get(ref, x + 1, b) + coef[ks] * self.get(ref, x - 1, b)
            res.append(r + coef[ke] * east + coef[kw] * west)
        return res

    def advance(self, src, x, lhs, dst, slope, y):
        v = self.row(src, x)
        t = [jnp.tanh(p) for p in v]
        p = self.mixed(lhs, t)
        s = self.stencil(src, x, v, 1)
        for b in range(self.blocks):
            self.put(slope, y, b, 1.0 - t[b] * t[b])
            self.put(dst, y, b, s[b] + p[b])


def over(count, bodies, after=None):
    def several(i, _):
        for body in bodies:
            body(i)
        if after is not None:
            after(i)
        return 0

    lax.fori_loop(0, count, several, 0)


def weights(mats, k, chans):
    return mats[k, 0:chans, 0 : 3 * chans].astype(BF16)


def collect(msg, tally, which, first, slots, table, list_v, list_s, sem, safe):
    sources = msg.shape[0]
    several = 8 if sources % 8 == 0 else 1

    def compact(i, off):
        blocks = [msg[i * several + r].T[first : first + slots] for r in range(several)]
        for r, block in enumerate(blocks):
            table[pl.ds(off, slots), 0:SUB] = block
            off = off + tally[i * several + r, which]
        return off

    count = lax.fori_loop(0, sources // several, compact, 0)
    lane = lax.broadcasted_iota(I32, (1, LANES), 1)

    def enlist(q, _):
        at = pl.multiple_of(q * LANES, LANES)
        code = table[pl.ds(at, LANES), :].T[SUB - 1 : SUB].astype(I32)
        list_v[pl.ds(q, 1)] = jnp.where(at + lane < count, code, safe)
        return 0

    lax.fori_loop(0, lax.shift_right_logical(count + LANES - 1, 7), enlist, 0)
    lists = pltpu.make_async_copy(list_v, list_s, sem)
    lists.start()
    return count, lists


def force(dense, count, table, list_s, stage, u1, u2, f1, f2):
    groups, blocks = dense.groups, dense.blocks
    shift = (WIDE.bit_length() - 1, blocks.bit_length() - 1, SUB.bit_length() - 1)

    def entry(i, r):
        q = list_s[lax.shift_right_logical(i, 4), lax.shift_left(i & 15, 3) + r]
        q = lax.shift_right_logical(q, shift[0])
        y = pl.multiple_of(lax.shift_left(q & (blocks - 1), 7), LANES)
        q = lax.shift_right_logical(q, shift[1])
        return lax.shift_right_logical(q, shift[2]), pl.ds(q & (SUB - 1), 1), pl.ds(y, WIDE)

    def gather(i, _):
        for r in range(SUB):
            x, at_s, at_y = entry(i, r)
            stage[0, i, r : r + 1] = u1[x, at_s, at_y]
            stage[1, i, r : r + 1] = u1[x + groups, at_s, at_y]
            stage[2, i, r : r + 1] = u2[x - groups, at_s, at_y]
            stage[3, i, r : r + 1] = u2[x, at_s, at_y]
        return 0

    turns = lax.shift_right_logical(count + SUB - 1, 3)
    lax.fori_loop(0, turns, gather, 0)

    per = 64
    lane1 = lax.broadcasted_iota(I32, (per, LANES), 1)
    nth = lax.broadcasted_iota(I32, (per, LANES), 0)

    def misfits(g, _):
        p = pl.multiple_of(g * per, per)
        at_p = pl.ds(pl.multiple_of(g * (per // SUB), per // SUB), per // SUB)
        rec = table[pl.ds(p, per)]
        wide = lambda k: jnp.broadcast_to(rec[:, k : k + 1], (per, LANES))
        valid = p + nth < count
        l = jnp.where(valid, wide(7).astype(I32) & (WIDE - 1), -WIDE)
        iw = [wide(k) for k in range(3, 7)]
        ws = []
        for h in range(2):
            here, nxt = lane1 == l - h * LANES, lane1 == l + (1 - h * LANES)
            ws.append([jnp.where(here, iw[k], jnp.where(nxt, iw[k + 1], 0.0)) for k in (0, 2)])
        w = wide(2)
        cut = lambda h: slice(h * LANES, (h + 1) * LANES)
        for t in range(2):
            q = 0.0
            for k in range(2):
                for h in range(2):
                    q = q + ws[h][k] * stage[2 * t + k, at_p, :, cut(h)].reshape(per, LANES)
            d = jnp.broadcast_to(jnp.sum(q, 1, keepdims=True), (per, LANES)) - wide(t)
            d = jnp.where(valid, w * d, 0.0)
            for k in range(2):
                for h in range(2):
                    stage[2 * t + k, at_p, :, cut(h)] = (d * ws[h][k]).reshape(per // SUB, SUB, LANES)
        return 0

    lax.fori_loop(0, lax.shift_right_logical(count + per - 1, 6), misfits, 0)

    def scatter(i, _):
        for r in range(SUB):
            x, at_s, at_y = entry(i, r)
            a = f1[x - groups, at_s, at_y] + stage[0, i, r : r + 1]
            b = f1[x, at_s, at_y] + stage[1, i, r : r + 1]
            c = f2[x - groups, at_s, at_y] + stage[2, i, r : r + 1]
            d = f2[x, at_s, at_y] + stage[3, i, r : r + 1]
            f1[x - groups, at_s, at_y] = a
            f1[x, at_s, at_y] = b
            f2[x - groups, at_s, at_y] = c
            f2[x, at_s, at_y] = d
        return 0

    lax.fori_loop(0, turns, scatter, 0)


def scatter_coefficients(coef, mats, dif, adv, mix, chans, levels):
    for ch in range(chans):
        i, j = ch // levels, ch % levels
        c, a, b = dif[j, i], adv[0, j, i], adv[1, j, i]
        for k, v in enumerate((c + a, c - a, c + b, c - b, 1.0 - 4.0 * c)):
            coef[k, ch : ch + 1, :] = jnp.full((1, LANES), v, F32)
    mats[2] = jnp.zeros((LANES, LANES), F32)
    m = mix[...]
    mats[2, 0:chans, 0:chans] = m
    mt = mats[2].T[0:chans, 0:chans]
    for k, v in enumerate((m, mt)):
        hi = v.astype(BF16).astype(F32)
        mats[k, 0:chans, 0:chans] = hi
        mats[k, 0:chans, chans : 2 * chans] = hi
        mats[k, 0:chans, 2 * chans : 3 * chans] = v - hi


def inner_kernel(
    dif, adv, u_hbm, b_hbm, mix, msg, u0, base, u1, u2, f1, f2, dt0, dt1, coef, mats,
    stage, table, code_v, code_s, list_v, list_s, sem_u, sem_b, sem_m, sem_l,
    *, rows, cols, chans, levels, slots,
):
    dense = Dense(coef, chans, cols)
    groups = dense.groups
    line = lambda ref, x: ref.at[pl.ds(x * groups, groups)]
    load_u = [pltpu.make_async_copy(u_hbm.at[:, :, x], line(u0, HALO + x), sem_u.at[x]) for x in range(rows)]
    load_b = [pltpu.make_async_copy(b_hbm.at[:, :, x], line(base, x), sem_b.at[x]) for x in range(rows)]
    for c in load_u + load_b:
        c.start()
    code_v[...] = msg[:, SUB - 1, :].astype(I32)
    codes = pltpu.make_async_copy(code_v, code_s, sem_m)
    codes.start()
    scatter_coefficients(coef, mats, dif, adv, mix, chans, levels)

    def clear(i):
        for ref in (f1, f2):
            ref[pl.ds(i * groups, groups)] = jnp.zeros((groups, SUB, cols), F32)

    over(rows + 6, [clear])
    codes.wait()
    count, lists = collect(
        msg, code_s, LANES - 1, 0, slots, table, list_v, list_s, sem_l, 8 * groups * SUB * dense.blocks * WIDE
    )
    fwd = weights(mats, 0, chans)
    for c in load_u:
        c.wait()
    half, half2 = (rows - 2) // 2, (rows - 4) // 2
    step = lambda off: lambda i: dense.advance(u0, off + i + 6, fwd, u1, dt0, off + i + 5)
    step2 = lambda off: lambda i: dense.advance(u1, off + i + 6, fwd, u2, dt1, off + i + 5)
    over(half, [step(0), step(half)])
    over(half2, [step2(0), step2(half2)])
    lists.wait()
    force(dense, count, table, list_s, stage, u1, u2, f1, f2)
    for c in load_b:
        c.wait()

    def departure(x):
        for b in range(dense.blocks):
            dense.put(base, x, b, dense.get(u0, x + HALO, b) - dense.get(base, x, b))

    over(rows, [departure])


def main_kernel(
    near_hbm, far_hbm, even_hbm, msg, u0_in, base_in, u1_in, u2_in, f1_in, f2_in, dt0_in, dt1_in, coef, mats,
    out_hbm, u0, base, u1, u2, f1, f2, dt0, dt1,
    stage, table, code_v, code_s, list_v, list_s, sem_e, sem_o, sem_m, sem_l,
    *, n, rows, cols, chans, slots, edge,
):
    dense = Dense(coef, chans, cols)
    groups, blocks = dense.groups, dense.blocks
    line = lambda ref, x: ref.at[pl.ds(x * groups, groups)]
    store_o = lambda x: pltpu.make_async_copy(line(base, x), out_hbm.at[:, :, x], sem_o.at[x])

    def clear(ref, x, count):
        ref[pl.ds(x * groups, count * groups)] = jnp.zeros((count * groups, SUB, cols), F32)

    me = lax.axis_index("gx")
    side, below = me & 1, HALO + rows
    start = (side * below + (1 - side) * (HALO - NEAR), side * (below + NEAR), (1 - side) * below)
    edges = []
    for k, (ref, x, count) in enumerate(zip((near_hbm, far_hbm, even_hbm), start, (NEAR, HALO - NEAR, HALO))):
        at = u0.at[pl.ds(x * groups, count * groups)]
        edges.append(pltpu.make_async_copy(ref, at, sem_e.at[k]))
    for c in edges:
        c.start()
    code_v[...] = msg[:, SUB - 1, :].astype(I32)
    codes = pltpu.make_async_copy(code_v, code_s, sem_m)
    codes.start()
    fwd, bwd = weights(mats, 0, chans), weights(mats, 1, chans)

    codes.wait()
    count, lists = collect(
        msg, code_s, LANES - 2, edge, slots, table, list_v, list_s, sem_l, 8 * groups * SUB * blocks * WIDE
    )
    for c in edges:
        c.wait()

    step = lambda off: lambda i: dense.advance(u0, off + 1 + i, fwd, u1, dt0, off + i)
    over(5, [step(0), step(rows + 3)])

    @pl.when(me == 0)
    def _():
        clear(u1, 0, 4)

    @pl.when(me == n - 1)
    def _():
        clear(u1, rows + 4, 4)

    step2 = lambda off: lambda i: dense.advance(u1, off + 1 + i, fwd, u2, dt1, off + i)
    over(5, [step2(0), step2(rows + 1)])

    lists.wait()
    force(dense, count, table, list_s, stage, u1, u2, f1, f2)

    def third(off):
        def body(i):
            k = off + i
            v = dense.row(f2, k)
            p = dense.mixed(bwd, v)
            s = dense.stencil(f2, k, v, -1)
            for b in range(blocks):
                dense.put(f1, k, b, (s[b] + dense.get(f1, k, b)) + dense.get(dt1, k, b) * p[b])

        return body

    half = (rows + 2) // 2
    over(half, [third(2), third(2 + half)])

    @pl.when(me == 0)
    def _():
        clear(f1, 2, 1)

    @pl.when(me == n - 1)
    def _():
        clear(f1, rows + 3, 1)

    def fourth(off):
        def body(i):
            x = off + i
            k = x + 3
            v = dense.row(f1, k)
            p = dense.mixed(bwd, v)
            s = dense.stencil(f1, k, v, -1)
            for b in range(blocks):
                r = s[b] + dense.get(dt0, x + 4, b) * p[b]
                dense.put(base, x, b, dense.get(base, x, b) + r)

        return body

    def store2(i):
        store_o(i).start()
        store_o(rows // 2 + i).start()

    over(rows // 2, [fourth(0), fourth(rows // 2)], store2)
    for x in range(rows):
        store_o(x).wait()


def shards(
    initial, background, mixing, diffusion, advection, obs_values, obs_weight, interp_weights,
    stencil_index, station_tile, counts,
):
    fields, levels, rows, cols = initial.shape
    chans = fields * levels
    groups = chans // SUB
    n = lax.axis_size("gx")
    held = obs_values.shape[1]
    cap = max(2, held * 3 // (2 * n))
    up8 = lambda x, k: -(-x // k) * k
    slots, edge_slots = up8(cap, SUB), up8(3 * cap, SUB)
    most, edge_most = up8(cap * n + slots, LANES), up8(3 * cap * n + edge_slots, LANES)
    in_hbm = lambda x: pltpu.with_memory_space_constraint(x, pltpu.HBM)
    u = in_hbm(initial.reshape(groups, SUB, rows, cols))
    b = in_hbm(background.reshape(groups, SUB, rows, cols))
    vmem, smem, hbm = (pl.BlockSpec(memory_space=s) for s in (pltpu.VMEM, pltpu.SMEM, pltpu.HBM))
    anywhere = pl.BlockSpec(memory_space=pl.ANY)
    buf = lambda count: pltpu.VMEM((count * groups, SUB, cols), F32)
    near_send, far_send, even_send, msg = pl.pallas_call(
        functools.partial(prep_kernel, n=n, rows=rows, cols=cols, groups=groups, edge=slots),
        out_shape=(buf(NEAR), buf(HALO - NEAR), buf(HALO), jax.ShapeDtypeStruct((n, SUB, LANES), F32)),
        in_specs=[hbm, vmem, vmem, vmem, vmem, vmem, smem],
        out_specs=(vmem, vmem, vmem, vmem),
        scratch_shapes=[pltpu.SemaphoreType.DMA((2 * HALO,))],
        compiler_params=pltpu.CompilerParams(vmem_limit_bytes=16 << 20),
        name="prep",
    )(u, *map(in_hbm, (obs_values, obs_weight, interp_weights, stencil_index, station_tile.T)), counts)
    swap = lambda first: [p for i in range(first, n - 1, 2) for p in ((i, i + 1), (i + 1, i))]
    near = lax.ppermute(near_send, "gx", swap(1))
    even = lax.ppermute(even_send, "gx", swap(0))
    msg = lax.all_to_all(msg, "gx", split_axis=0, concat_axis=0, tiled=True)
    far = lax.ppermute(far_send, "gx", swap(1))
    records = lambda most: [
        pltpu.VMEM((4, most // SUB, SUB, WIDE), F32),
        pltpu.VMEM((most, LANES), F32),
        pltpu.VMEM((n, LANES), I32),
        pltpu.SMEM((n, LANES), I32),
        pltpu.VMEM((most // LANES, LANES), I32),
        pltpu.SMEM((most // LANES, LANES), I32),
    ]
    dma = pltpu.SemaphoreType.DMA
    bufs = [buf(rows + k) for k in (2 * HALO, 0, 8, 6, 6, 6, 8, 6)]
    ready = pl.pallas_call(
        functools.partial(inner_kernel, rows=rows, cols=cols, chans=chans, levels=levels, slots=slots),
        out_shape=(*bufs, pltpu.VMEM((5, chans, LANES), F32), pltpu.VMEM((3, LANES, LANES), F32)),
        in_specs=[smem, smem, hbm, hbm, vmem, vmem],
        out_specs=[vmem] * 10,
        scratch_shapes=records(most) + [dma((rows,)), dma((rows,)), dma(()), dma(())],
        compiler_params=pltpu.CompilerParams(vmem_limit_bytes=12 << 20),
        name="inner",
    )(in_hbm(diffusion.T), in_hbm(advection.transpose(0, 2, 1)), u, b, in_hbm(mixing), msg)
    out = pl.pallas_call(
        functools.partial(main_kernel, n=n, rows=rows, cols=cols, chans=chans, slots=edge_slots, edge=slots),
        out_shape=(jax.ShapeDtypeStruct(u.shape, F32), *bufs),
        in_specs=[anywhere, anywhere, anywhere, *[vmem] * 11],
        out_specs=[hbm, *[vmem] * 8],
        input_output_aliases={4 + k: 1 + k for k in range(8)},
        scratch_shapes=records(edge_most) + [dma((3,)), dma((rows,)), dma(()), dma(())],
        compiler_params=pltpu.CompilerParams(vmem_limit_bytes=12 << 20),
        name="adjoint",
    )(near, far, even, msg, *ready)[0]
    return out.reshape(fields, levels, rows, cols)


def solution(mesh):
    placed = (
        P("groups", None, "gx", None),
        P("groups", None, "gx", None),
        P(),
        P(),
        P(),
        P("groups", "gx"),
        P("groups", "gx"),
        P("groups", "gx"),
        P("groups", "gx"),
        P("gx", "groups"),
        P("groups", "gx"),
    )
    return jax.shard_map(
        shards, mesh=mesh, in_specs=placed, out_specs=P("groups", None, "gx", None), check_vma=False
    )
```

```python
import functools

import jax
import jax.numpy as jnp
from jax import lax
from jax.experimental import pallas as pl
from jax.experimental.pallas import tpu as pltpu
from jax.sharding import PartitionSpec as P

HALO = 5
NEAR = 3
LANES = 128
WIDE = 2 * LANES
SUB = 8
F32, BF16, I32 = jnp.float32, jnp.bfloat16, jnp.int32


def split3(x):
    hi = x.astype(BF16).astype(F32)
    mid = (x - hi).astype(BF16).astype(F32)
    return [hi, mid, x - hi - mid]


def prep_kernel(
    u_hbm, val_hbm, wgt_hbm, iw_hbm, cell_hbm, tile_hbm, cnt, near, far, even, msg,
    val, wgt, iw, cell, tile, sem, sem_r, *, n, rows, cols, groups, edge,
):
    parity = lax.axis_index("gx") & 1
    last = rows - HALO
    small = zip((val_hbm, wgt_hbm, iw_hbm, cell_hbm, tile_hbm), (val, wgt, iw, cell, tile))
    records = [pltpu.make_async_copy(src, dst, sem_r.at[k]) for k, (src, dst) in enumerate(small)]
    copies = []
    start = (parity * (rows - NEAR), parity * last + (1 - parity) * NEAR, (1 - parity) * last)
    for ref, x, count in zip((near, far, even), start, (NEAR, HALO - NEAR, HALO)):
        for k in range(count):
            at = ref.at[pl.ds(k * groups, groups)]
            copies.append(pltpu.make_async_copy(u_hbm.at[:, :, x + k], at, sem.at[len(copies)]))
    for c in records + copies:
        c.start()
    for c in records:
        c.wait()
    held = val.shape[1]
    blocks = cols // LANES
    tgt = tile[...]
    lane = lax.broadcasted_iota(I32, (1, held), 1)
    live = lane < cnt[0, 0]
    base = cell[0:1, :]
    plane = rows * cols
    chan = base // plane
    rest = base - chan * plane
    row = rest // cols
    col = rest - row * cols
    blk = jnp.minimum(col // LANES, blocks - 2)
    line = (row + 4) * groups + chan // SUB
    code = ((line * SUB + chan % SUB) * blocks + blk) * WIDE + col - blk * LANES
    step = rows * groups * SUB * blocks * WIDE
    feats = jnp.concatenate(split3(jnp.concatenate([val[...], wgt[...], iw[...], jnp.zeros((1, held), F32)], 0)), 0)
    pad = jnp.zeros((SUB - 3, held), F32)
    dest = lax.broadcasted_iota(I32, (n, held), 0)
    low, high = row <= 1, row >= rows - 3
    own = (tgt == dest) & live
    near = live & ((tgt == dest + 1) & low | (tgt == dest - 1) & high)
    outer = near | own & (low | high)
    within = own & (row >= 2) & (row <= rows - 4)
    hits = jnp.concatenate([within.astype(F32), outer.astype(F32)], 0)
    tri = lax.broadcasted_iota(I32, (held, held), 0) < lax.broadcasted_iota(I32, (held, held), 1)
    rank = jnp.dot(hits.astype(BF16), tri.astype(F32).astype(BF16), preferred_element_type=F32)
    place = jnp.where(within, rank[0:n], jnp.where(outer, rank[n:] + float(edge), -1.0))
    total = jnp.sum(hits, axis=1, keepdims=True)
    slot = lax.broadcasted_iota(I32, (LANES, held), 0).astype(F32)
    sub8 = lax.broadcasted_iota(I32, (SUB, LANES), 0)
    lane8 = lax.broadcasted_iota(I32, (SUB, LANES), 1)
    for d in range(n):
        pick = (place[d : d + 1, :] == slot).astype(F32).astype(BF16)
        code_d = (code + (tgt - d) * step).astype(F32)
        lhs = jnp.concatenate([feats, *split3(code_d), pad], 0).astype(BF16)
        got = lax.dot_general(lhs, pick, (((1,), (1,)), ((), ())), preferred_element_type=F32)
        where = got[24:25] + got[25:26] + got[26:27]
        got = got[0:8] + got[8:16] + got[16:24]
        got = jnp.where(sub8 == 7, where, got)
        got = jnp.where((sub8 == 7) & (lane8 == LANES - 1), total[d : d + 1, 0:1], got)
        msg[d] = jnp.where((sub8 == 7) & (lane8 == LANES - 2), total[n + d : n + d + 1, 0:1], got)
    for c in copies:
        c.wait()


class Dense:
    def __init__(self, coef, chans, cols):
        self.coef, self.chans, self.cols = coef, chans, cols
        self.groups, self.blocks = chans // SUB, cols // LANES

    def get(self, ref, x, b):
        v = ref[pl.ds(x * self.groups, self.groups), :, b * LANES : (b + 1) * LANES]
        return v.reshape(self.chans, LANES)

    def row(self, ref, x):
        return [self.get(ref, x, b) for b in range(self.blocks)]

    def put(self, ref, x, b, v):
        at = pl.ds(x * self.groups, self.groups)
        ref[at, :, b * LANES : (b + 1) * LANES] = v.reshape(self.groups, SUB, LANES)

    def mixed(self, lhs, parts):
        res = []
        for b in range(0, self.blocks, 2):
            v = jnp.concatenate(parts[b : b + 2], 1)
            hi = v.astype(BF16).astype(F32)
            rhs = jnp.concatenate([hi, v - hi, hi], 0).astype(BF16)
            r = jnp.dot(lhs, rhs, preferred_element_type=F32)
            res += [r[:, :LANES], r[:, LANES:]]
        return res

    def stencil(self, ref, x, parts, sign):
        coef = self.coef
        lane = lax.broadcasted_iota(I32, (self.chans, LANES), 1)
        zero = jnp.zeros((self.chans, LANES), F32)
        kn, ks, ke, kw = (0, 1, 2, 3) if sign > 0 else (1, 0, 3, 2)
        res = []
        left = [pltpu.roll(v, LANES - 1, 1) for v in parts] + [zero]
        right = [zero] + [pltpu.roll(v, 1, 1) for v in parts]
        for b in range(self.blocks):
            east = jnp.where(lane == LANES - 1, left[b + 1], left[b])
            west = jnp.where(lane == 0, right[b], right[b + 1])
            r = coef[4] * parts[b] + coef[kn] * self.get(ref, x + 1, b) + coef[ks] * self.get(ref, x - 1, b)
            res.append(r + coef[ke] * east + coef[kw] * west)
        return res

    def advance(self, src, x, lhs, dst, slope, y):
        v = self.row(src, x)
        t = [jnp.tanh(p) for p in v]
        p = self.mixed(lhs, t)
        s = self.stencil(src, x, v, 1)
        for b in range(self.blocks):
            self.put(slope, y, b, 1.0 - t[b] * t[b])
            self.put(dst, y, b, s[b] + p[b])


def over(count, bodies, after=None):
    def several(i, _):
        for body in bodies:
            body(i)
        if after is not None:
            after(i)
        return 0

    lax.fori_loop(0, count, several, 0)


def spans(count, most):
    ways = max(k for k in range(1, most + 1) if count % k == 0)
    return range(0, count, count // ways), count // ways


def weights(mats, k, chans):
    return mats[k, 0:chans, 0 : 3 * chans].astype(BF16)


def collect(msg, tally, which, first, slots, table, list_v, list_s, sem, safe):
    sources = msg.shape[0]
    several = 8 if sources % 8 == 0 else 1

    def compact(i, off):
        blocks = [msg[i * several + r].T[first : first + slots] for r in range(several)]
        for r, block in enumerate(blocks):
            table[pl.ds(off, slots), 0:SUB] = block
            off = off + tally[i * several + r, which]
        return off

    count = lax.fori_loop(0, sources // several, compact, 0)
    lane = lax.broadcasted_iota(I32, (1, LANES), 1)

    def enlist(q, _):
        at = pl.multiple_of(q * LANES, LANES)
        code = table[pl.ds(at, LANES), :].T[SUB - 1 : SUB].astype(I32)
        list_v[pl.ds(q, 1)] = jnp.where(at + lane < count, code, safe)
        return 0

    lax.fori_loop(0, lax.shift_right_logical(count + LANES - 1, 7), enlist, 0)
    lists = pltpu.make_async_copy(list_v, list_s, sem)
    lists.start()
    return count, lists


def force(dense, count, table, list_s, stage, u1, u2, f1, f2):
    groups, blocks = dense.groups, dense.blocks
    shift = (WIDE.bit_length() - 1, blocks.bit_length() - 1, SUB.bit_length() - 1)

    def entry(i, r):
        q = list_s[lax.shift_right_logical(i, 4), lax.shift_left(i & 15, 3) + r]
        q = lax.shift_right_logical(q, shift[0])
        y = pl.multiple_of(lax.shift_left(q & (blocks - 1), 7), LANES)
        q = lax.shift_right_logical(q, shift[1])
        return lax.shift_right_logical(q, shift[2]), pl.ds(q & (SUB - 1), 1), pl.ds(y, WIDE)

    def gather(i, _):
        for r in range(SUB):
            x, at_s, at_y = entry(i, r)
            stage[0, i, r : r + 1] = u1[x, at_s, at_y]
            stage[1, i, r : r + 1] = u1[x + groups, at_s, at_y]
            stage[2, i, r : r + 1] = u2[x - groups, at_s, at_y]
            stage[3, i, r : r + 1] = u2[x, at_s, at_y]
        return 0

    turns = lax.shift_right_logical(count + SUB - 1, 3)
    lax.fori_loop(0, turns, gather, 0)

    per = 64
    lane1 = lax.broadcasted_iota(I32, (per, LANES), 1)
    nth = lax.broadcasted_iota(I32, (per, LANES), 0)

    def misfits(g, _):
        p = pl.multiple_of(g * per, per)
        at_p = pl.ds(pl.multiple_of(g * (per // SUB), per // SUB), per // SUB)
        rec = table[pl.ds(p, per)]
        wide = lambda k: jnp.broadcast_to(rec[:, k : k + 1], (per, LANES))
        valid = p + nth < count
        l = jnp.where(valid, wide(7).astype(I32) & (WIDE - 1), -WIDE)
        iw = [wide(k) for k in range(3, 7)]
        ws = []
        for h in range(2):
            here, nxt = lane1 == l - h * LANES, lane1 == l + (1 - h * LANES)
            ws.append([jnp.where(here, iw[k], jnp.where(nxt, iw[k + 1], 0.0)) for k in (0, 2)])
        w = wide(2)
        cut = lambda h: slice(h * LANES, (h + 1) * LANES)
        for t in range(2):
            q = 0.0
            for k in range(2):
                for h in range(2):
                    q = q + ws[h][k] * stage[2 * t + k, at_p, :, cut(h)].reshape(per, LANES)
            d = jnp.broadcast_to(jnp.sum(q, 1, keepdims=True), (per, LANES)) - wide(t)
            d = jnp.where(valid, w * d, 0.0)
            for k in range(2):
                for h in range(2):
                    stage[2 * t + k, at_p, :, cut(h)] = (d * ws[h][k]).reshape(per // SUB, SUB, LANES)
        return 0

    lax.fori_loop(0, lax.shift_right_logical(count + per - 1, 6), misfits, 0)

    def scatter(i, _):
        for r in range(SUB):
            x, at_s, at_y = entry(i, r)
            a = f1[x - groups, at_s, at_y] + stage[0, i, r : r + 1]
            b = f1[x, at_s, at_y] + stage[1, i, r : r + 1]
            c = f2[x - groups, at_s, at_y] + stage[2, i, r : r + 1]
            d = f2[x, at_s, at_y] + stage[3, i, r : r + 1]
            f1[x - groups, at_s, at_y] = a
            f1[x, at_s, at_y] = b
            f2[x - groups, at_s, at_y] = c
            f2[x, at_s, at_y] = d
        return 0

    lax.fori_loop(0, turns, scatter, 0)


def scatter_coefficients(coef, mats, dif, adv, mix, chans, levels):
    for ch in range(chans):
        i, j = ch // levels, ch % levels
        c, a, b = dif[j, i], adv[0, j, i], adv[1, j, i]
        for k, v in enumerate((c + a, c - a, c + b, c - b, 1.0 - 4.0 * c)):
            coef[k, ch : ch + 1, :] = jnp.full((1, LANES), v, F32)
    mats[2] = jnp.zeros((LANES, LANES), F32)
    m = mix[...]
    mats[2, 0:chans, 0:chans] = m
    mt = mats[2].T[0:chans, 0:chans]
    for k, v in enumerate((m, mt)):
        hi = v.astype(BF16).astype(F32)
        mats[k, 0:chans, 0:chans] = hi
        mats[k, 0:chans, chans : 2 * chans] = hi
        mats[k, 0:chans, 2 * chans : 3 * chans] = v - hi


def inner_kernel(
    dif, adv, u_hbm, b_hbm, mix, msg, u0, base, u1, u2, f1, f2, dt0, dt1, coef, mats,
    stage, table, code_v, code_s, list_v, list_s, sem_u, sem_b, sem_m, sem_l,
    *, rows, cols, chans, levels, slots,
):
    dense = Dense(coef, chans, cols)
    groups = dense.groups
    line = lambda ref, x: ref.at[pl.ds(x * groups, groups)]
    load_u = [pltpu.make_async_copy(u_hbm.at[:, :, x], line(u0, HALO + x), sem_u.at[x]) for x in range(rows)]
    load_b = [pltpu.make_async_copy(b_hbm.at[:, :, x], line(base, x), sem_b.at[x]) for x in range(rows)]
    for c in load_u + load_b:
        c.start()
    code_v[...] = msg[:, SUB - 1, :].astype(I32)
    codes = pltpu.make_async_copy(code_v, code_s, sem_m)
    codes.start()
    scatter_coefficients(coef, mats, dif, adv, mix, chans, levels)

    def clear(i):
        for ref in (f1, f2):
            ref[pl.ds(i * groups, groups)] = jnp.zeros((groups, SUB, cols), F32)

    over(rows + 6, [clear])
    codes.wait()
    count, lists = collect(
        msg, code_s, LANES - 1, 0, slots, table, list_v, list_s, sem_l, 8 * groups * SUB * dense.blocks * WIDE
    )
    fwd = weights(mats, 0, chans)
    for c in load_u:
        c.wait()
    (at, part), (at2, part2) = spans(rows - 2, 7), spans(rows - 4, 4)
    step = lambda off: lambda i: dense.advance(u0, off + i + 6, fwd, u1, dt0, off + i + 5)
    step2 = lambda off: lambda i: dense.advance(u1, off + i + 6, fwd, u2, dt1, off + i + 5)
    over(part, [step(k) for k in at])
    over(part2, [step2(k) for k in at2])
    lists.wait()
    force(dense, count, table, list_s, stage, u1, u2, f1, f2)
    for c in load_b:
        c.wait()

    def departure(x):
        for b in range(dense.blocks):
            dense.put(base, x, b, dense.get(u0, x + HALO, b) - dense.get(base, x, b))

    over(rows, [departure])


def main_kernel(
    near_hbm, far_hbm, even_hbm, msg, u0_in, base_in, u1_in, u2_in, f1_in, f2_in, dt0_in, dt1_in, coef, mats,
    out_hbm, u0, base, u1, u2, f1, f2, dt0, dt1,
    stage, table, code_v, code_s, list_v, list_s, sem_e, sem_o, sem_m, sem_l,
    *, n, rows, cols, chans, slots, edge,
):
    dense = Dense(coef, chans, cols)
    groups, blocks = dense.groups, dense.blocks
    line = lambda ref, x: ref.at[pl.ds(x * groups, groups)]
    store_o = lambda x: pltpu.make_async_copy(line(base, x), out_hbm.at[:, :, x], sem_o.at[x])

    def clear(ref, x, count):
        ref[pl.ds(x * groups, count * groups)] = jnp.zeros((count * groups, SUB, cols), F32)

    me = lax.axis_index("gx")
    side, below = me & 1, HALO + rows
    start = (side * below + (1 - side) * (HALO - NEAR), side * (below + NEAR), (1 - side) * below)
    edges = []
    for k, (ref, x, count) in enumerate(zip((near_hbm, far_hbm, even_hbm), start, (NEAR, HALO - NEAR, HALO))):
        at = u0.at[pl.ds(x * groups, count * groups)]
        edges.append(pltpu.make_async_copy(ref, at, sem_e.at[k]))
    for c in edges:
        c.start()
    code_v[...] = msg[:, SUB - 1, :].astype(I32)
    codes = pltpu.make_async_copy(code_v, code_s, sem_m)
    codes.start()
    fwd, bwd = weights(mats, 0, chans), weights(mats, 1, chans)

    codes.wait()
    count, lists = collect(
        msg, code_s, LANES - 2, edge, slots, table, list_v, list_s, sem_l, 8 * groups * SUB * blocks * WIDE
    )
    for c in edges:
        c.wait()

    step = lambda off: lambda i: dense.advance(u0, off + 1 + i, fwd, u1, dt0, off + i)
    over(1, [step(k + b) for k in range(5) for b in (0, rows + 3)])

    @pl.when(me == 0)
    def _():
        clear(u1, 0, 4)

    @pl.when(me == n - 1)
    def _():
        clear(u1, rows + 4, 4)

    step2 = lambda off: lambda i: dense.advance(u1, off + 1 + i, fwd, u2, dt1, off + i)
    over(1, [step2(k + b) for k in range(5) for b in (0, rows + 1)])

    lists.wait()
    force(dense, count, table, list_s, stage, u1, u2, f1, f2)

    def third(off):
        def body(i):
            k = off + i
            v = dense.row(f2, k)
            p = dense.mixed(bwd, v)
            s = dense.stencil(f2, k, v, -1)
            for b in range(blocks):
                dense.put(f1, k, b, (s[b] + dense.get(f1, k, b)) + dense.get(dt1, k, b) * p[b])

        return body

    at, part = spans(rows + 2, 6)
    over(part, [third(2 + k) for k in at])

    @pl.when(me == 0)
    def _():
        clear(f1, 2, 1)

    @pl.when(me == n - 1)
    def _():
        clear(f1, rows + 3, 1)

    def fourth(off):
        def body(i):
            x = off + i
            k = x + 3
            v = dense.row(f1, k)
            p = dense.mixed(bwd, v)
            s = dense.stencil(f1, k, v, -1)
            for b in range(blocks):
                r = s[b] + dense.get(dt0, x + 4, b) * p[b]
                dense.put(base, x, b, dense.get(base, x, b) + r)

        return body

    quarters, quarter = spans(rows, 4)

    def store2(i):
        for k in quarters:
            store_o(k + i).start()

    over(quarter, [fourth(k) for k in quarters], store2)
    for x in range(rows):
        store_o(x).wait()


def shards(
    initial, background, mixing, diffusion, advection, obs_values, obs_weight, interp_weights,
    stencil_index, station_tile, counts,
):
    fields, levels, rows, cols = initial.shape
    chans = fields * levels
    groups = chans // SUB
    n = lax.axis_size("gx")
    held = obs_values.shape[1]
    cap = max(2, held * 3 // (2 * n))
    up8 = lambda x, k: -(-x // k) * k
    slots, edge_slots = up8(cap, SUB), up8(3 * cap, SUB)
    most, edge_most = up8(cap * n + slots, LANES), up8(3 * cap * n + edge_slots, LANES)
    in_hbm = lambda x: pltpu.with_memory_space_constraint(x, pltpu.HBM)
    u = in_hbm(initial.reshape(groups, SUB, rows, cols))
    b = in_hbm(background.reshape(groups, SUB, rows, cols))
    vmem, smem, hbm = (pl.BlockSpec(memory_space=s) for s in (pltpu.VMEM, pltpu.SMEM, pltpu.HBM))
    anywhere = pl.BlockSpec(memory_space=pl.ANY)
    buf = lambda count: pltpu.VMEM((count * groups, SUB, cols), F32)
    near_send, far_send, even_send, msg = pl.pallas_call(
        functools.partial(prep_kernel, n=n, rows=rows, cols=cols, groups=groups, edge=slots),
        out_shape=(buf(NEAR), buf(HALO - NEAR), buf(HALO), jax.ShapeDtypeStruct((n, SUB, LANES), F32)),
        in_specs=[*[hbm] * 6, smem],
        out_specs=(vmem, vmem, vmem, vmem),
        scratch_shapes=[
            *[pltpu.VMEM(a.shape, a.dtype) for a in (obs_values, obs_weight, interp_weights, stencil_index)],
            pltpu.VMEM((1, held), I32),
            pltpu.SemaphoreType.DMA((2 * HALO,)),
            pltpu.SemaphoreType.DMA((5,)),
        ],
        compiler_params=pltpu.CompilerParams(vmem_limit_bytes=16 << 20),
        name="prep",
    )(u, *map(in_hbm, (obs_values, obs_weight, interp_weights, stencil_index, station_tile.T)), counts)
    swap = lambda first: [p for i in range(first, n - 1, 2) for p in ((i, i + 1), (i + 1, i))]
    near = lax.ppermute(near_send, "gx", swap(1))
    even = lax.ppermute(even_send, "gx", swap(0))
    msg = lax.all_to_all(msg, "gx", split_axis=0, concat_axis=0, tiled=True)
    far = lax.ppermute(far_send, "gx", swap(1))
    records = lambda most: [
        pltpu.VMEM((4, most // SUB, SUB, WIDE), F32),
        pltpu.VMEM((most, LANES), F32),
        pltpu.VMEM((n, LANES), I32),
        pltpu.SMEM((n, LANES), I32),
        pltpu.VMEM((most // LANES, LANES), I32),
        pltpu.SMEM((most // LANES, LANES), I32),
    ]
    dma = pltpu.SemaphoreType.DMA
    bufs = [buf(rows + k) for k in (2 * HALO, 0, 8, 6, 6, 6, 8, 6)]
    ready = pl.pallas_call(
        functools.partial(inner_kernel, rows=rows, cols=cols, chans=chans, levels=levels, slots=slots),
        out_shape=(*bufs, pltpu.VMEM((5, chans, LANES), F32), pltpu.VMEM((3, LANES, LANES), F32)),
        in_specs=[smem, smem, hbm, hbm, vmem, vmem],
        out_specs=[vmem] * 10,
        scratch_shapes=records(most) + [dma((rows,)), dma((rows,)), dma(()), dma(())],
        compiler_params=pltpu.CompilerParams(vmem_limit_bytes=12 << 20),
        name="inner",
    )(in_hbm(diffusion.T), in_hbm(advection.transpose(0, 2, 1)), u, b, in_hbm(mixing), msg)
    out = pl.pallas_call(
        functools.partial(main_kernel, n=n, rows=rows, cols=cols, chans=chans, slots=edge_slots, edge=slots),
        out_shape=(jax.ShapeDtypeStruct(u.shape, F32), *bufs),
        in_specs=[anywhere, anywhere, anywhere, *[vmem] * 11],
        out_specs=[hbm, *[vmem] * 8],
        input_output_aliases={4 + k: 1 + k for k in range(8)},
        scratch_shapes=records(edge_most) + [dma((3,)), dma((rows,)), dma(()), dma(())],
        compiler_params=pltpu.CompilerParams(vmem_limit_bytes=12 << 20),
        name="adjoint",
    )(near, far, even, msg, *ready)[0]
    return out.reshape(fields, levels, rows, cols)


def solution(mesh):
    placed = (
        P("groups", None, "gx", None),
        P("groups", None, "gx", None),
        P(),
        P(),
        P(),
        P("groups", "gx"),
        P("groups", "gx"),
        P("groups", "gx"),
        P("groups", "gx"),
        P("gx", "groups"),
        P("groups", "gx"),
    )
    return jax.shard_map(
        shards, mesh=mesh, in_specs=placed, out_specs=P("groups", None, "gx", None), check_vma=False
    )
```
